32 devices in a mesh: dp: 8 (over z, x), section: 4 (over y, core).
Axes of the slice: x: 2, y: 2, z: 4, core: 2. Of those that a mesh axis runs over, the one named last changes fastest.
Arguments:
- entry_tokens: bfloat16 [8, 8, 16, 8192], P('dp'), may hold values from -6 to 6
- section_norm_gain: bfloat16 [4, 8192], P('section'), may hold values from 0.5 to 1.5
- adapter_down_weight: bfloat16 [4, 48, 8192], P('section'), may hold values from -0.0625 to 0.0625
- adapter_up_weight: bfloat16 [4, 48, 8192], P('section'), may hold values from -0.875 to 0.875
- output_gradient: bfloat16 [8, 8, 16, 8192], P('dp'), may hold values from -6 to 6
- lengths: int32 [8, 8], P('dp'), may hold values from 1 to 16
- keep: int32 [8, 4, 8, 16], P('dp', 'section'), may hold values from 0 to 1, as said below
Outputs:
- grad_up: float32 [4, 48, 8192], P('section')
- grad_gain: float32 [4, 8192], P('section')
The draws below stay inside these ranges and needn't reach their ends.
Inputs may be any that keep to these rules, and one draw needn't show every extreme that they name: `keep`: 0 or 1; token 0 of every microbatch is kept at every section.
All inputs are finite; a program needn't handle non-finite values.
Results may differ from the reference program's by a relative error of at most 0.02.
Values may be sent and summed in bfloat16 or wider, within the bound.
No kernel may reach another device: no remote copies, remote signals or barrier semaphores. Data moves between devices by JAX's collectives and lax.ppermute only.
A program may use at most 64 MiB of HBM per device.

```python
import jax
import jax.numpy as jnp
from jax import lax

HIDDEN_WIDTH = 8192
ADAPTER_RANK = 48
TOK = 16
MICRO = 8
RELAY_SECTIONS = 4
GROUPS = 8


def draw_keep(key, part):
    ticket = jax.random.randint(key, (GROUPS, RELAY_SECTIONS, MICRO, TOK), 0, 5 * RELAY_SECTIONS)
    section_number = jnp.arange(RELAY_SECTIONS, dtype=jnp.int32)[None, :, None, None]
    limit = RELAY_SECTIONS + 3 * section_number
    position = jnp.arange(TOK, dtype=jnp.int32)[None, None, None, :]
    return jnp.where((ticket < limit) | (position == 0), 1, 0).astype(jnp.int32)


def touch_ends(array, key, least, high):
    spot = [jax.random.randint(jax.random.fold_in(key, axis), (), 0, length) for axis, length in enumerate(array.shape)]
    main_axis = array.shape.index(max(array.shape))
    neighbour = spot[:main_axis] + [(spot[main_axis] + 1) % array.shape[main_axis]] + spot[main_axis + 1:]
    return array.at[tuple(spot)].set(least).at[tuple(neighbour)].set(high)


def levels(key, extent, cuts, least, top_value):
    factor_of = 1.0
    for dim, shards_of in cuts:
        draws = jax.random.uniform(jax.random.fold_in(jax.random.fold_in(key, 6), dim), (shards_of,), jnp.float32, least / len(cuts), top_value / len(cuts))
        factor_of = factor_of * jnp.repeat(jnp.exp(draws), extent[dim] // shards_of).reshape((-1,) + (1,) * (len(extent) - 1 - dim))
    return factor_of


def noise(key, extent, spread, most, split=(), kind=jnp.bfloat16):
    values = jax.random.normal(key, extent, jnp.float32) * spread
    if len(split) > 0:
        values = levels(key, extent, split, -0.22, 0.18) * values
    return jnp.clip(values, min=-most, max=most).astype(kind)


def setup_inputs(seed: int = 0) -> dict:
    key_of = jax.random.split(jax.random.key(seed), 8)
    return {
        "entry_tokens": noise(key_of[0], (GROUPS, MICRO, TOK, HIDDEN_WIDTH), 1.0, 6.0, ((0, 8),)),
        "section_norm_gain": jnp.clip(1.0 + 0.1 * jax.random.normal(key_of[1], (RELAY_SECTIONS, HIDDEN_WIDTH), jnp.float32), 0.5, 1.5).astype(jnp.bfloat16),
        "adapter_down_weight": noise(key_of[2], (RELAY_SECTIONS, ADAPTER_RANK, HIDDEN_WIDTH), HIDDEN_WIDTH ** -0.5, 0.0625, ((0, 4),)),
        "adapter_up_weight": noise(key_of[3], (RELAY_SECTIONS, ADAPTER_RANK, HIDDEN_WIDTH), ADAPTER_RANK ** -0.5, 0.875, ((0, 4),)),
        "output_gradient": noise(key_of[4], (GROUPS, MICRO, TOK, HIDDEN_WIDTH), 1.0, 6.0, ((0, 8),)),
        "lengths": touch_ends(jax.random.randint(key_of[5], (GROUPS, MICRO), 1, TOK + 1), jax.random.fold_in(key_of[5], 1), 1, TOK).astype(jnp.int32),
        "keep": draw_keep(jax.random.fold_in(key_of[7], 71), 0),
    }


EPS = 1e-05

def forward_section(current_rows, gain_row, down_rows, up_rows, kept_rows):
    widened_rows = current_rows.astype(jnp.float32)
    inverse_norm = lax.rsqrt(lax.optimization_barrier(jnp.mean(widened_rows * widened_rows, axis=-1, keepdims=True)) + EPS)
    normed = (widened_rows * inverse_norm * gain_row.astype(jnp.float32)).astype(jnp.bfloat16)
    lowrank_rows = jnp.einsum('uwko,bo->uwkb', normed.astype(jnp.float32), down_rows.astype(jnp.float32)).astype(jnp.bfloat16)
    branch = jnp.einsum('jvau,ui->jvai', lowrank_rows.astype(jnp.float32), up_rows.astype(jnp.float32))
    weight = kept_rows[..., None]
    section_output = (widened_rows + weight * branch).astype(jnp.bfloat16)
    energy = lax.optimization_barrier(jnp.sum(weight * branch * branch, axis=(2, 3)))
    return (section_output, lowrank_rows, inverse_norm, widened_rows, energy)

def reference(entry_tokens, section_norm_gain, adapter_down_weight, adapter_up_weight, output_gradient, lengths, keep):
    position = jnp.arange(TOK, dtype=jnp.int32)
    valid_mask = (position[None, None, :] < lengths[:, :, None]).astype(jnp.float32)
    retained_mask = keep.astype(jnp.float32) * valid_mask[:, None]
    input_per_section = []
    energy = jnp.zeros((GROUPS, MICRO), jnp.float32)
    current_rows = entry_tokens
    for section_number in range(RELAY_SECTIONS):
        input_per_section.append(current_rows)
        current_rows, lowrank_rows, inverse_norm, widened_rows, section_power = forward_section(current_rows, section_norm_gain[section_number], adapter_down_weight[section_number], adapter_up_weight[section_number], retained_mask[:, section_number])
        energy = energy + section_power
    count = lax.optimization_barrier(jnp.sum(retained_mask, axis=(1, 3)))
    scaling = 1.0 / (count * jnp.sqrt(energy / (HIDDEN_WIDTH * count) + EPS))
    cotangent = (output_gradient.astype(jnp.float32) * valid_mask[..., None] * scaling[:, :, None, None]).astype(jnp.bfloat16)
    grads_up = []
    grads_gain = []
    for section_number in reversed(range(RELAY_SECTIONS)):
        section_output, lowrank_rows, inverse_norm, widened_rows, section_power = forward_section(input_per_section[section_number], section_norm_gain[section_number], adapter_down_weight[section_number], adapter_up_weight[section_number], retained_mask[:, section_number])
        weight = retained_mask[:, section_number][..., None]
        branch_gradient = (weight * cotangent.astype(jnp.float32)).astype(jnp.bfloat16)
        grad_section = jnp.einsum('gmtr,gmtd->rd', lowrank_rows.astype(jnp.float32), branch_gradient.astype(jnp.float32))
        lowrank_gradient = jnp.einsum('uwko,bo->uwkb', branch_gradient.astype(jnp.float32), adapter_up_weight[section_number].astype(jnp.float32)).astype(jnp.bfloat16)
        norm_gradient = jnp.einsum('jvau,ui->jvai', lowrank_gradient.astype(jnp.float32), adapter_down_weight[section_number].astype(jnp.float32))
        gain_grad = lax.optimization_barrier(jnp.sum(norm_gradient * widened_rows * inverse_norm, axis=(0, 1, 2)))
        scaled = norm_gradient * section_norm_gain[section_number].astype(jnp.float32)
        input_grad = inverse_norm * scaled - widened_rows * inverse_norm ** 3 * lax.optimization_barrier(jnp.mean(scaled * widened_rows, axis=-1, keepdims=True))
        cotangent = (cotangent.astype(jnp.float32) + input_grad).astype(jnp.bfloat16)
        grads_up.append(grad_section)
        grads_gain.append(gain_grad)
    grad_up = jnp.stack(grads_up[::-1])
    grad_gain = jnp.stack(grads_gain[::-1])
    return (grad_up, grad_gain)
```

```python
import jax
import jax.numpy as jnp
from jax import lax
from jax.experimental import pallas as pl
from jax.experimental.pallas import tpu as pltpu
from jax.sharding import PartitionSpec as P

EPS = 1e-05


def passed_along(block, axis, distance):
    devices = range(lax.axis_size(axis))
    route = [(i - distance, i) for i in devices if i - distance in devices]
    return lax.ppermute(block, axis, route)


def section_apply(current_rows, gain_f32, down_rows, up_rows, weight):
    widened_rows = current_rows.astype(jnp.float32)
    inverse_norm = lax.rsqrt(jnp.mean(widened_rows * widened_rows, axis=-1, keepdims=True) + EPS)
    normed = (widened_rows * inverse_norm * gain_f32).astype(jnp.bfloat16)
    lowrank_rows = lax.dot_general(
        normed, down_rows, (((1,), (1,)), ((), ())), preferred_element_type=jnp.float32
    ).astype(jnp.bfloat16)
    branch = jnp.dot(lowrank_rows, up_rows, preferred_element_type=jnp.float32)
    section_output = (widened_rows + weight * branch).astype(jnp.bfloat16)
    row_energy = jnp.sum(weight * branch * branch, axis=1)
    return (section_output, lowrank_rows, row_energy)


def relay_body(
    entry_tokens,
    section_norm_gain,
    adapter_down_weight,
    adapter_up_weight,
    output_gradient,
    lengths,
    keep,
):
    section_total = lax.axis_size("section")
    section_index = lax.axis_index("section")
    micro_count = entry_tokens.shape[1]
    token_count = entry_tokens.shape[2]
    model_width = entry_tokens.shape[3]
    rank_total = adapter_down_weight.shape[1]
    group_size = 2
    block_count = micro_count // group_size
    block_rows = group_size * token_count
    gain_f32 = section_norm_gain[0].astype(jnp.float32)
    down_rows = adapter_down_weight[0]
    up_rows = adapter_up_weight[0]
    position = jnp.arange(token_count, dtype=jnp.int32)
    valid_mask = (position[None, :] < lengths[0][:, None]).astype(jnp.float32)
    retained_mask = keep[0, 0].astype(jnp.float32) * valid_mask
    count_local = jnp.sum(retained_mask, axis=1)
    tick_count = block_count + section_total - 1
    block_ids = jnp.arange(block_count, dtype=jnp.int32)
    tokens_blocks = entry_tokens[0].reshape(block_count, block_rows, model_width)
    grad_blocks = output_gradient[0].reshape(block_count, block_rows, model_width)
    kept_blocks = retained_mask.reshape(block_count, block_rows)
    valid_blocks = valid_mask.reshape(block_count, block_rows)

    def forward_tick(step_index, state_tuple):
        incoming, stashed, low_stash, energy = state_tuple
        block_index = step_index - section_index
        active = (block_index >= 0) & (block_index < block_count)
        slot_index = jnp.clip(block_index, 0, block_count - 1)
        fresh_rows = lax.dynamic_index_in_dim(tokens_blocks, slot_index, 0, keepdims=False)
        current_rows = jnp.where(section_index == 0, fresh_rows, incoming)
        weight = lax.dynamic_index_in_dim(kept_blocks, slot_index, 0, keepdims=False)[:, None]
        section_output, lowrank_rows, row_energy = section_apply(
            current_rows, gain_f32, down_rows, up_rows, weight
        )
        block_energy = jnp.sum(row_energy.reshape(group_size, token_count), axis=1)
        old_rows = lax.dynamic_index_in_dim(stashed, slot_index, 0, keepdims=False)
        stashed = lax.dynamic_update_index_in_dim(
            stashed, jnp.where(active, current_rows, old_rows), slot_index, 0
        )
        old_low = lax.dynamic_index_in_dim(low_stash, slot_index, 0, keepdims=False)
        low_stash = lax.dynamic_update_index_in_dim(
            low_stash, jnp.where(active, lowrank_rows, old_low), slot_index, 0
        )
        energy = (
            energy + (block_ids == block_index).astype(jnp.float32)[:, None] * block_energy[None, :]
        )
        passed = passed_along(section_output, "section", 1)
        return (passed, stashed, low_stash, energy)

    start_state = (
        jnp.zeros((block_rows, model_width), jnp.bfloat16),
        jnp.zeros((block_count, block_rows, model_width), jnp.bfloat16),
        jnp.zeros((block_count, block_rows, rank_total), jnp.bfloat16),
        jnp.zeros((block_count, group_size), jnp.float32),
    )
    ignored, stashed, low_stash, energy_blocks = lax.fori_loop(
        0, tick_count, forward_tick, start_state
    )
    energy = energy_blocks.reshape(micro_count)
    total_energy, total_count = lax.psum((energy, count_local), "section")
    scaling = 1.0 / (total_count * jnp.sqrt(total_energy / (model_width * total_count) + EPS))
    scaling_rows = (scaling[:, None] * jnp.ones((1, token_count), jnp.float32)).reshape(
        block_count, block_rows
    )

    def backward_tick(step_index, state_tuple):
        incoming, grad_stash, gain_grad = state_tuple
        block_index = step_index - (section_total - 1 - section_index)
        active = (block_index >= 0) & (block_index < block_count)
        slot_index = jnp.clip(block_index, 0, block_count - 1)
        valid_row = lax.dynamic_index_in_dim(valid_blocks, slot_index, 0, keepdims=False)[:, None]
        scale_row = lax.dynamic_index_in_dim(scaling_rows, slot_index, 0, keepdims=False)[:, None]
        seed_rows = (
            lax.dynamic_index_in_dim(grad_blocks, slot_index, 0, keepdims=False).astype(jnp.float32)
            * valid_row
            * scale_row
        ).astype(jnp.bfloat16)
        cotangent = jnp.where(section_index == section_total - 1, seed_rows, incoming)
        current_rows = lax.dynamic_index_in_dim(stashed, slot_index, 0, keepdims=False)
        weight = lax.dynamic_index_in_dim(kept_blocks, slot_index, 0, keepdims=False)[:, None]
        widened_rows = current_rows.astype(jnp.float32)
        inverse_norm = lax.rsqrt(
            jnp.mean(widened_rows * widened_rows, axis=-1, keepdims=True) + EPS
        )
        branch_gradient = (weight * cotangent.astype(jnp.float32)).astype(jnp.bfloat16)
        lowrank_gradient = lax.dot_general(
            branch_gradient, up_rows, (((1,), (1,)), ((), ())), preferred_element_type=jnp.float32
        ).astype(jnp.bfloat16)
        norm_gradient = jnp.dot(lowrank_gradient, down_rows, preferred_element_type=jnp.float32)
        gain_grad = gain_grad + jnp.where(
            active, jnp.sum(norm_gradient * widened_rows * inverse_norm, axis=0), 0.0
        )
        scaled = norm_gradient * gain_f32
        input_grad = inverse_norm * scaled - widened_rows * inverse_norm**3 * jnp.mean(
            scaled * widened_rows, axis=-1, keepdims=True
        )
        updated = (cotangent.astype(jnp.float32) + input_grad).astype(jnp.bfloat16)
        old_rows = lax.dynamic_index_in_dim(grad_stash, slot_index, 0, keepdims=False)
        grad_stash = lax.dynamic_update_index_in_dim(
            grad_stash, jnp.where(active, branch_gradient, old_rows), slot_index, 0
        )
        passed = passed_along(updated, "section", -1)
        return (passed, grad_stash, gain_grad)

    back_state = (
        jnp.zeros((block_rows, model_width), jnp.bfloat16),
        jnp.zeros((block_count, block_rows, model_width), jnp.bfloat16),
        jnp.zeros((model_width,), jnp.float32),
    )
    ignored, grad_stash, gain_grad = lax.fori_loop(0, tick_count, backward_tick, back_state)
    low_rows = low_stash.reshape(micro_count * token_count, rank_total)
    grad_rows = grad_stash.reshape(micro_count * token_count, model_width)
    grad_section = lax.dot_general(
        low_rows, grad_rows, (((0,), (0,)), ((), ())), preferred_element_type=jnp.float32
    )
    summed_up, summed_gain = lax.psum((grad_section, gain_grad), "dp")
    return (summed_up[None], summed_gain[None])


LANES = 128
PIECES = 4
VMEM_BUDGET = 56 * 1024 * 1024


def swapped(block, axis, bit):
    route = [(i, i ^ bit) for i in range(lax.axis_size(axis))]
    return lax.ppermute(block, axis, route)


def rank_space_kernel(
    index_ref, masks_ref, tokens_hbm, grads_hbm, *rest, sections, rank, width, micro, tokens, parts
):
    weights_hbm = rest[:sections]
    down_hbm, payload_ref, stack, down, gram, proj, branch_stash, turned, sems = rest[sections:]
    rows = micro * tokens
    span = stack.shape[0] - 2 * rows
    half = span // 2
    model_width = stack.shape[1]
    piece = model_width // PIECES
    own = index_ref[0]
    copies = []
    for p in range(PIECES):
        columns = pl.ds(p * piece, piece)
        group = [
            pltpu.make_async_copy(
                tokens_hbm.at[:, columns], stack.at[pl.ds(span, rows), columns], sems.at[p, 0]
            ),
            pltpu.make_async_copy(
                grads_hbm.at[:, columns], stack.at[pl.ds(span + rows, rows), columns], sems.at[p, 1]
            ),
        ]
        for k in range(sections):
            start = pl.multiple_of((own ^ k) * rank, 16)
            for q in range(2):
                group.append(
                    pltpu.make_async_copy(
                        weights_hbm[k].at[pl.ds(q * rank, rank), columns],
                        stack.at[pl.ds(q * half + start, rank), columns],
                        sems.at[p, 2 + 2 * k + q],
                    )
                )
        for copy in group:
            copy.start()
        copies.append(group)
    down_copy = pltpu.make_async_copy(down_hbm, down, sems.at[0, 2 + 2 * sections])
    down_copy.start()
    used = sections * rank
    for q in range(2):
        if used < half:
            stack[q * half + used : (q + 1) * half, :] = jnp.zeros(
                (half - used, model_width), jnp.bfloat16
            )
    square = jnp.zeros((rows, LANES), jnp.float32)
    for p in range(PIECES):
        for copy in copies[p]:
            copy.wait()
        columns = slice(p * piece, (p + 1) * piece)
        product = lax.dot_general(
            stack[half:, columns],
            stack[:span, columns],
            (((1,), (1,)), ((), ())),
            preferred_element_type=jnp.float32,
        )
        if p == 0:
            gram[...] = product[:half]
            proj[...] = product[half:]
        else:
            gram[...] += product[:half]
            proj[...] += product[half:]
        for j in range(piece // LANES):
            lane = p * piece + j * LANES
            values = stack[span : span + rows, lane : lane + LANES].astype(jnp.float32)
            square += values * values
    norm_sq = jnp.sum(square, axis=1, keepdims=True)

    lane_ids = lax.broadcasted_iota(jnp.int32, (rows, half), 1)
    blocks = [(lane_ids >= s * rank) & (lane_ids < (s + 1) * rank) for s in range(sections)]
    kept = [masks_ref[:, s : s + 1] for s in range(sections)]
    valid = masks_ref[:, sections : sections + 1]
    gram_hi = gram[...].astype(jnp.bfloat16)
    gram_lo = (gram[...] - gram_hi.astype(jnp.float32)).astype(jnp.bfloat16)
    down_side = proj[:rows, :half]
    up_side = proj[:rows, half:]
    down_saved = jnp.zeros((rows, half), jnp.float32)
    kept_low = jnp.zeros((rows, half), jnp.float32)
    power = jnp.zeros((rows, 1), jnp.float32)
    count = jnp.zeros((rows, 1), jnp.float32)
    inverses = []
    for s in range(sections):
        inverse = lax.rsqrt(norm_sq / width + EPS)
        inverses.append(inverse)
        masked = jnp.where(blocks[s], down_side, 0.0)
        down_saved += masked
        low = (masked * inverse).astype(jnp.bfloat16)
        low_f32 = low.astype(jnp.float32)
        kept_low += kept[s] * low_f32
        branch_stash[s] = up_side
        moved = jnp.dot(low, gram_hi, preferred_element_type=jnp.float32) + jnp.dot(
            low, gram_lo, preferred_element_type=jnp.float32
        )
        energy = jnp.sum(low_f32 * moved[:, half:], axis=1, keepdims=True)
        cross = jnp.sum(low_f32 * up_side, axis=1, keepdims=True)
        power += kept[s] * energy
        count += kept[s]
        norm_sq = jnp.maximum(norm_sq + kept[s] * (2.0 * cross + energy), 0.0)
        down_side = down_side + kept[s] * moved[:, :half]
        up_side = up_side + kept[s] * moved[:, half:]

    def per_micro(column):
        wide = jnp.broadcast_to(column, (rows, LANES)).reshape(micro, tokens, LANES)
        total = jnp.broadcast_to(jnp.sum(wide, axis=1, keepdims=True), wide.shape)
        return total.reshape(rows, LANES)[:, :1]

    total_energy = jnp.maximum(per_micro(power), 0.0)
    total_count = per_micro(count)
    scaling = 1.0 / (total_count * jnp.sqrt(total_energy / (width * total_count) + EPS))
    alpha = valid * scaling

    carried = alpha * proj[rows:, half:]
    scaled_grad = jnp.zeros((rows, half), jnp.float32)
    later = jnp.zeros((rows, half), jnp.float32)
    weights = [None] * sections
    zero = jnp.zeros((rows, 1), jnp.float32)
    beta = zero
    for s in reversed(range(sections)):
        lowgrad = jnp.where(blocks[s], kept[s] * carried, 0.0).astype(jnp.bfloat16)
        lowgrad_f32 = lowgrad.astype(jnp.float32)
        mean = jnp.sum(lowgrad_f32 * down_saved, axis=1, keepdims=True) / width
        inverse = inverses[s]
        pull = inverse * inverse * inverse * mean
        weights[s] = pull
        scaled = inverse * lowgrad_f32
        scaled_grad += scaled
        if s > 0:
            back = lax.dot_general(
                lowgrad, gram_hi[:, :half], (((1,), (1,)), ((), ())), preferred_element_type=jnp.float32
            ) + lax.dot_general(
                lowgrad, gram_lo[:, :half], (((1,), (1,)), ((), ())), preferred_element_type=jnp.float32
            )
            carried = carried + inverse * back - pull * branch_stash[s]

    beta = zero
    gamma = jnp.zeros((rows, half), jnp.float32)
    for s in reversed(range(sections)):
        gamma = jnp.where(blocks[s], beta, gamma)
        beta = beta + jnp.where(s > own, weights[s], zero)
    low_edge = own * rank
    high_edge = low_edge + rank
    after = jnp.where(lane_ids >= high_edge, scaled_grad, 0.0).astype(jnp.bfloat16)
    before = jnp.where(lane_ids < low_edge, kept_low, 0.0).astype(jnp.bfloat16)
    pulled = (gamma * kept_low).astype(jnp.bfloat16)
    turned[0] = (alpha * kept_low).T
    turned[1] = (-beta * kept_low).T
    turned[2] = kept_low.T
    turned[3] = scaled_grad.T
    mine = pl.ds(pl.multiple_of(low_edge, 16), rank)
    low_own = turned[2, mine, :].astype(jnp.bfloat16)
    grad_own = turned[3, mine, :].astype(jnp.bfloat16)
    coef_up = [
        turned[1, mine, :].astype(jnp.bfloat16),
        turned[0, mine, :].astype(jnp.bfloat16),
        jnp.dot(low_own, after, preferred_element_type=jnp.float32).astype(jnp.bfloat16),
        -jnp.dot(low_own, pulled, preferred_element_type=jnp.float32).astype(jnp.bfloat16),
    ]
    coef_gain = [
        grad_own,
        jnp.dot(grad_own, before, preferred_element_type=jnp.float32).astype(jnp.bfloat16),
    ]
    left = jnp.concatenate(
        [
            jnp.concatenate([coef_up[2], coef_up[3], coef_up[0], coef_up[1]], axis=1),
            jnp.concatenate(
                [
                    jnp.zeros((rank, half), jnp.bfloat16),
                    coef_gain[1],
                    coef_gain[0],
                    jnp.zeros((rank, rows), jnp.bfloat16),
                ],
                axis=1,
            ),
        ],
        axis=0,
    )
    down_copy.wait()
    chunk = model_width // parts
    lane_blocks = chunk // LANES
    tail = payload_ref.shape[1] - lane_blocks * rank
    for c in range(parts):
        columns = slice(c * chunk, (c + 1) * chunk)
        result = jnp.dot(left, stack[:, columns], preferred_element_type=jnp.float32)
        gain = jnp.sum(
            result[rank:] * down[:, columns].astype(jnp.float32), axis=0, keepdims=True
        )
        for j in range(lane_blocks):
            payload_ref[c, j * rank : (j + 1) * rank, :] = result[
                :rank, j * LANES : (j + 1) * LANES
            ].astype(jnp.bfloat16)
        gain_rows = [gain[:, j * LANES : (j + 1) * LANES] for j in range(lane_blocks)]
        gain_rows.append(jnp.zeros((tail - lane_blocks, LANES), jnp.float32))
        payload_ref[c, lane_blocks * rank :, :] = jnp.concatenate(gain_rows, axis=0).astype(
            jnp.bfloat16
        )


def sum_kernel(parts_ref, out_ref):
    total = parts_ref[0].astype(jnp.float32)
    for c in range(1, parts_ref.shape[0]):
        total += parts_ref[c].astype(jnp.float32)
    rounded = total.astype(jnp.bfloat16)
    for c in range(out_ref.shape[0]):
        out_ref[c] = rounded


def unpack_kernel(parts_ref, up_ref, gain_ref):
    parts = parts_ref.shape[0]
    rank = up_ref.shape[0]
    chunk = up_ref.shape[1] // parts
    lane_blocks = chunk // LANES
    for c in range(parts):
        tail = parts_ref[c, lane_blocks * rank :, :].astype(jnp.float32)
        for j in range(lane_blocks):
            lanes = slice(c * chunk + j * LANES, c * chunk + (j + 1) * LANES)
            up_ref[:, lanes] = parts_ref[c, j * rank : (j + 1) * rank, :].astype(jnp.float32)
            gain_ref[:, lanes] = tail[j : j + 1, :]


def rank_space_body(
    entry_tokens,
    section_norm_gain,
    adapter_down_weight,
    adapter_up_weight,
    output_gradient,
    lengths,
    keep,
):
    sections = lax.axis_size("section")
    parts = lax.axis_size("dp")
    section_index = lax.axis_index("section")
    micro, tokens, width = entry_tokens.shape[1:]
    rank = adapter_down_weight.shape[1]
    rows = micro * tokens
    down = adapter_down_weight[0]
    scaled_down = (
        section_norm_gain[0].astype(jnp.float32) * down.astype(jnp.float32)
    ).astype(jnp.bfloat16)
    weights = [jnp.concatenate([scaled_down, adapter_up_weight[0]], axis=0)]
    bit = 1
    while bit < sections:
        fresh = swapped(weights[0], "section", bit)
        more = [fresh]
        for k in range(1, bit):
            more.append(swapped(fresh, "section", k))
        weights = weights + more
        bit *= 2
    valid = (jnp.arange(tokens, dtype=jnp.int32)[None, :] < lengths[0][:, None]).astype(jnp.float32)
    kept_all = lax.all_gather(keep[0, 0], "section").astype(jnp.float32) * valid[None]
    masks = jnp.concatenate([kept_all.reshape(sections, rows), valid.reshape(1, rows)], axis=0).T
    half = -(-sections * rank // LANES) * LANES
    lane_blocks = width // parts // LANES
    payload_rows = lane_blocks * rank + -(-lane_blocks // 16) * 16
    hbm = pl.BlockSpec(memory_space=pltpu.MemorySpace.HBM)
    vmem = pl.BlockSpec(memory_space=pltpu.MemorySpace.VMEM)
    payload = pl.pallas_call(
        lambda *refs: rank_space_kernel(
            *refs,
            sections=sections,
            rank=rank,
            width=width,
            micro=micro,
            tokens=tokens,
            parts=parts,
        ),
        out_shape=jax.ShapeDtypeStruct((parts, payload_rows, LANES), jnp.bfloat16),
        in_specs=[pl.BlockSpec(memory_space=pltpu.MemorySpace.SMEM), vmem] + [hbm] * (sections + 3),
        out_specs=vmem,
        scratch_shapes=[
            pltpu.VMEM((2 * half + 2 * rows, width), jnp.bfloat16),
            pltpu.VMEM((rank, width), jnp.bfloat16),
            pltpu.VMEM((half, 2 * half), jnp.float32),
            pltpu.VMEM((2 * rows, 2 * half), jnp.float32),
            pltpu.VMEM((sections, rows, half), jnp.float32),
            pltpu.VMEM((4, half, rows), jnp.float32),
            pltpu.SemaphoreType.DMA((PIECES, 3 + 2 * sections)),
        ],
        compiler_params=pltpu.CompilerParams(vmem_limit_bytes=VMEM_BUDGET),
        name="rank_space",
    )(
        section_index.astype(jnp.int32).reshape(1),
        masks,
        entry_tokens.reshape(rows, width),
        output_gradient.reshape(rows, width),
        *weights,
        down,
    )
    spread = lax.all_to_all(payload, "dp", 0, 0, tiled=True)
    summed = pl.pallas_call(
        sum_kernel,
        out_shape=jax.ShapeDtypeStruct(payload.shape, jnp.bfloat16),
        in_specs=[vmem],
        out_specs=vmem,
        name="sum_parts",
    )(spread)
    gathered = lax.all_to_all(summed, "dp", 0, 0, tiled=True)
    grad_up, grad_gain = pl.pallas_call(
        unpack_kernel,
        out_shape=(
            jax.ShapeDtypeStruct((rank, width), jnp.float32),
            jax.ShapeDtypeStruct((1, width), jnp.float32),
        ),
        in_specs=[vmem],
        out_specs=(vmem, vmem),
        name="unpack",
    )(gathered)
    return (grad_up[None], grad_gain)


def fits_rank_space(args, sections, parts):
    micro, tokens, width = args[0].shape[1:]
    rank = args[2].shape[1]
    rows = micro * tokens
    half = -(-sections * rank // LANES) * LANES
    return (
        sections & (sections - 1) == 0
        and width % (parts * LANES) == 0
        and width % (PIECES * LANES) == 0
        and rank % 16 == 0
        and rows % LANES == 0
        and tokens % 8 == 0
        and (2 * half + 2 * rows) * width * 2 <= VMEM_BUDGET // 3
    )


def body(*args):
    if fits_rank_space(args, lax.axis_size("section"), lax.axis_size("dp")):
        return rank_space_body(*args)
    return relay_body(*args)


def solution(mesh):
    in_specs = (
        P("dp", None, None, None),
        P("section", None),
        P("section", None, None),
        P("section", None, None),
        P("dp", None, None, None),
        P("dp", None),
        P("dp", "section", None, None),
    )
    out_specs = (P("section", None, None), P("section", None))
    return jax.shard_map(body, mesh=mesh, in_specs=in_specs, out_specs=out_specs, check_vma=False)
```

```python
import jax
import jax.numpy as jnp
from jax import lax
from jax.experimental import pallas as pl
from jax.experimental.pallas import tpu as pltpu
from jax.sharding import PartitionSpec as P

EPS = 1e-05


def passed_along(block, axis, distance):
    devices = range(lax.axis_size(axis))
    route = [(i - distance, i) for i in devices if i - distance in devices]
    return lax.ppermute(block, axis, route)


def section_apply(current_rows, gain_f32, down_rows, up_rows, weight):
    widened_rows = current_rows.astype(jnp.float32)
    inverse_norm = lax.rsqrt(jnp.mean(widened_rows * widened_rows, axis=-1, keepdims=True) + EPS)
    normed = (widened_rows * inverse_norm * gain_f32).astype(jnp.bfloat16)
    lowrank_rows = lax.dot_general(
        normed, down_rows, (((1,), (1,)), ((), ())), preferred_element_type=jnp.float32
    ).astype(jnp.bfloat16)
    branch = jnp.dot(lowrank_rows, up_rows, preferred_element_type=jnp.float32)
    section_output = (widened_rows + weight * branch).astype(jnp.bfloat16)
    row_energy = jnp.sum(weight * branch * branch, axis=1)
    return (section_output, lowrank_rows, row_energy)


def relay_body(
    entry_tokens,
    section_norm_gain,
    adapter_down_weight,
    adapter_up_weight,
    output_gradient,
    lengths,
    keep,
):
    section_total = lax.axis_size("section")
    section_index = lax.axis_index("section")
    micro_count = entry_tokens.shape[1]
    token_count = entry_tokens.shape[2]
    model_width = entry_tokens.shape[3]
    rank_total = adapter_down_weight.shape[1]
    group_size = 2
    block_count = micro_count // group_size
    block_rows = group_size * token_count
    gain_f32 = section_norm_gain[0].astype(jnp.float32)
    down_rows = adapter_down_weight[0]
    up_rows = adapter_up_weight[0]
    position = jnp.arange(token_count, dtype=jnp.int32)
    valid_mask = (position[None, :] < lengths[0][:, None]).astype(jnp.float32)
    retained_mask = keep[0, 0].astype(jnp.float32) * valid_mask
    count_local = jnp.sum(retained_mask, axis=1)
    tick_count = block_count + section_total - 1
    block_ids = jnp.arange(block_count, dtype=jnp.int32)
    tokens_blocks = entry_tokens[0].reshape(block_count, block_rows, model_width)
    grad_blocks = output_gradient[0].reshape(block_count, block_rows, model_width)
    kept_blocks = retained_mask.reshape(block_count, block_rows)
    valid_blocks = valid_mask.reshape(block_count, block_rows)

    def forward_tick(step_index, state_tuple):
        incoming, stashed, low_stash, energy = state_tuple
        block_index = step_index - section_index
        active = (block_index >= 0) & (block_index < block_count)
        slot_index = jnp.clip(block_index, 0, block_count - 1)
        fresh_rows = lax.dynamic_index_in_dim(tokens_blocks, slot_index, 0, keepdims=False)
        current_rows = jnp.where(section_index == 0, fresh_rows, incoming)
        weight = lax.dynamic_index_in_dim(kept_blocks, slot_index, 0, keepdims=False)[:, None]
        section_output, lowrank_rows, row_energy = section_apply(
            current_rows, gain_f32, down_rows, up_rows, weight
        )
        block_energy = jnp.sum(row_energy.reshape(group_size, token_count), axis=1)
        old_rows = lax.dynamic_index_in_dim(stashed, slot_index, 0, keepdims=False)
        stashed = lax.dynamic_update_index_in_dim(
            stashed, jnp.where(active, current_rows, old_rows), slot_index, 0
        )
        old_low = lax.dynamic_index_in_dim(low_stash, slot_index, 0, keepdims=False)
        low_stash = lax.dynamic_update_index_in_dim(
            low_stash, jnp.where(active, lowrank_rows, old_low), slot_index, 0
        )
        energy = (
            energy + (block_ids == block_index).astype(jnp.float32)[:, None] * block_energy[None, :]
        )
        passed = passed_along(section_output, "section", 1)
        return (passed, stashed, low_stash, energy)

    start_state = (
        jnp.zeros((block_rows, model_width), jnp.bfloat16),
        jnp.zeros((block_count, block_rows, model_width), jnp.bfloat16),
        jnp.zeros((block_count, block_rows, rank_total), jnp.bfloat16),
        jnp.zeros((block_count, group_size), jnp.float32),
    )
    ignored, stashed, low_stash, energy_blocks = lax.fori_loop(
        0, tick_count, forward_tick, start_state
    )
    energy = energy_blocks.reshape(micro_count)
    total_energy, total_count = lax.psum((energy, count_local), "section")
    scaling = 1.0 / (total_count * jnp.sqrt(total_energy / (model_width * total_count) + EPS))
    scaling_rows = (scaling[:, None] * jnp.ones((1, token_count), jnp.float32)).reshape(
        block_count, block_rows
    )

    def backward_tick(step_index, state_tuple):
        incoming, grad_stash, gain_grad = state_tuple
        block_index = step_index - (section_total - 1 - section_index)
        active = (block_index >= 0) & (block_index < block_count)
        slot_index = jnp.clip(block_index, 0, block_count - 1)
        valid_row = lax.dynamic_index_in_dim(valid_blocks, slot_index, 0, keepdims=False)[:, None]
        scale_row = lax.dynamic_index_in_dim(scaling_rows, slot_index, 0, keepdims=False)[:, None]
        seed_rows = (
            lax.dynamic_index_in_dim(grad_blocks, slot_index, 0, keepdims=False).astype(jnp.float32)
            * valid_row
            * scale_row
        ).astype(jnp.bfloat16)
        cotangent = jnp.where(section_index == section_total - 1, seed_rows, incoming)
        current_rows = lax.dynamic_index_in_dim(stashed, slot_index, 0, keepdims=False)
        weight = lax.dynamic_index_in_dim(kept_blocks, slot_index, 0, keepdims=False)[:, None]
        widened_rows = current_rows.astype(jnp.float32)
        inverse_norm = lax.rsqrt(
            jnp.mean(widened_rows * widened_rows, axis=-1, keepdims=True) + EPS
        )
        branch_gradient = (weight * cotangent.astype(jnp.float32)).astype(jnp.bfloat16)
        lowrank_gradient = lax.dot_general(
            branch_gradient, up_rows, (((1,), (1,)), ((), ())), preferred_element_type=jnp.float32
        ).astype(jnp.bfloat16)
        norm_gradient = jnp.dot(lowrank_gradient, down_rows, preferred_element_type=jnp.float32)
        gain_grad = gain_grad + jnp.where(
            active, jnp.sum(norm_gradient * widened_rows * inverse_norm, axis=0), 0.0
        )
        scaled = norm_gradient * gain_f32
        input_grad = inverse_norm * scaled - widened_rows * inverse_norm**3 * jnp.mean(
            scaled * widened_rows, axis=-1, keepdims=True
        )
        updated = (cotangent.astype(jnp.float32) + input_grad).astype(jnp.bfloat16)
        old_rows = lax.dynamic_index_in_dim(grad_stash, slot_index, 0, keepdims=False)
        grad_stash = lax.dynamic_update_index_in_dim(
            grad_stash, jnp.where(active, branch_gradient, old_rows), slot_index, 0
        )
        passed = passed_along(updated, "section", -1)
        return (passed, grad_stash, gain_grad)

    back_state = (
        jnp.zeros((block_rows, model_width), jnp.bfloat16),
        jnp.zeros((block_count, block_rows, model_width), jnp.bfloat16),
        jnp.zeros((model_width,), jnp.float32),
    )
    ignored, grad_stash, gain_grad = lax.fori_loop(0, tick_count, backward_tick, back_state)
    low_rows = low_stash.reshape(micro_count * token_count, rank_total)
    grad_rows = grad_stash.reshape(micro_count * token_count, model_width)
    grad_section = lax.dot_general(
        low_rows, grad_rows, (((0,), (0,)), ((), ())), preferred_element_type=jnp.float32
    )
    summed_up, summed_gain = lax.psum((grad_section, gain_grad), "dp")
    return (summed_up[None], summed_gain[None])


LANES = 128
PIECES = 8
EDGE = 3
VMEM_BUDGET = 56 * 1024 * 1024


def swapped(block, axis, bit):
    route = [(i, i ^ bit) for i in range(lax.axis_size(axis))]
    return lax.ppermute(block, axis, route)


def rank_space_kernel(
    index_ref, masks_ref, *rest, regions, sections, rank, width, micro, tokens, parts
):
    sources = rest[: len(regions)]
    down_hbm = rest[len(regions)]
    payload_refs = rest[len(regions) + 1 : len(regions) + 1 + parts]
    stack, down, gram, proj, branch_stash, turned, sems, down_sem = rest[len(regions) + 1 + parts :]
    rows = micro * tokens
    span = stack.shape[0] - 2 * rows
    half = span // 2
    model_width = stack.shape[1]
    piece = model_width // PIECES
    own = index_ref[0]
    side = index_ref[1]
    place = index_ref[2]
    near = side * (PIECES - EDGE) * piece
    away = (1 - side) * (PIECES - EDGE) * piece
    starts = [near + p * piece for p in range(EDGE)]
    starts += [(EDGE + p) * piece for p in range(PIECES - 2 * EDGE)]
    starts += [away + p * piece for p in range(EDGE)]
    starts = [pl.multiple_of(start, LANES) for start in starts]
    copies = []
    for p in range(PIECES):
        group = []
        for index, (kind, first, last, where) in enumerate(regions):
            if not first <= p < last:
                continue
            source = sources[index]
            lanes = starts[p] if where else (p - first) * piece
            columns = pl.ds(lanes, piece)
            if kind in ("tokens", "grads"):
                top = span + (rows if kind == "grads" else 0)
                moves = [(0, top, rows)]
            else:
                start = pl.multiple_of((own ^ kind[0]) * rank, 16)
                moves = [
                    (i * rank, pl.multiple_of(q * half + start, 16), rank)
                    for i, q in enumerate(kind[1])
                ]
            for from_row, to_row, count in moves:
                group.append(
                    pltpu.make_async_copy(
                        source.at[pl.ds(from_row, count), columns],
                        stack.at[pl.ds(to_row, count), pl.ds(starts[p], piece)],
                        sems.at[p, len(group)],
                    )
                )
        for copy in group:
            copy.start()
        copies.append(group)
    down_copy = pltpu.make_async_copy(down_hbm, down, down_sem)
    down_copy.start()
    used = sections * rank
    for q in range(2):
        if used < half:
            stack[q * half + used : (q + 1) * half, :] = jnp.zeros(
                (half - used, model_width), jnp.bfloat16
            )
    square = jnp.zeros((rows, LANES), jnp.float32)
    for p in range(PIECES):
        for copy in copies[p]:
            copy.wait()
        columns = pl.ds(starts[p], piece)
        product = lax.dot_general(
            stack[half:, columns],
            stack[:span, columns],
            (((1,), (1,)), ((), ())),
            preferred_element_type=jnp.float32,
        )
        if p == 0:
            gram[...] = product[:half]
            proj[...] = product[half:]
        else:
            gram[...] += product[:half]
            proj[...] += product[half:]
        values = stack[span : span + rows, columns].astype(jnp.float32)
        for j in range(piece // LANES):
            part = values[:, j * LANES : (j + 1) * LANES]
            square += part * part
    norm_sq = jnp.sum(square, axis=1, keepdims=True)

    lane_ids = lax.broadcasted_iota(jnp.int32, (rows, half), 1)
    blocks = [(lane_ids >= s * rank) & (lane_ids < (s + 1) * rank) for s in range(sections)]
    kept = [masks_ref[:, s : s + 1] for s in range(sections)]
    valid = masks_ref[:, sections : sections + 1]
    gram_hi = gram[...].astype(jnp.bfloat16)
    gram_lo = (gram[...] - gram_hi.astype(jnp.float32)).astype(jnp.bfloat16)
    down_side = proj[:rows, :half]
    up_side = proj[:rows, half:]
    down_saved = jnp.zeros((rows, half), jnp.float32)
    kept_low = jnp.zeros((rows, half), jnp.float32)
    power = jnp.zeros((rows, 1), jnp.float32)
    count = jnp.zeros((rows, 1), jnp.float32)
    inverses = []
    for s in range(sections):
        inverse = lax.rsqrt(norm_sq / width + EPS)
        inverses.append(inverse)
        masked = jnp.where(blocks[s], down_side, 0.0)
        down_saved += masked
        low = (masked * inverse).astype(jnp.bfloat16)
        low_f32 = low.astype(jnp.float32)
        kept_low += kept[s] * low_f32
        branch_stash[s] = up_side
        moved = jnp.dot(low, gram_hi, preferred_element_type=jnp.float32) + jnp.dot(
            low, gram_lo, preferred_element_type=jnp.float32
        )
        energy = jnp.sum(low_f32 * moved[:, half:], axis=1, keepdims=True)
        cross = jnp.sum(low_f32 * up_side, axis=1, keepdims=True)
        power += kept[s] * energy
        count += kept[s]
        norm_sq = jnp.maximum(norm_sq + kept[s] * (2.0 * cross + energy), 0.0)
        down_side = down_side + kept[s] * moved[:, :half]
        up_side = up_side + kept[s] * moved[:, half:]

    def per_micro(column):
        wide = jnp.broadcast_to(column, (rows, LANES)).reshape(micro, tokens, LANES)
        total = jnp.broadcast_to(jnp.sum(wide, axis=1, keepdims=True), wide.shape)
        return total.reshape(rows, LANES)[:, :1]

    total_energy = jnp.maximum(per_micro(power), 0.0)
    total_count = per_micro(count)
    scaling = 1.0 / (total_count * jnp.sqrt(total_energy / (width * total_count) + EPS))
    alpha = valid * scaling

    carried = alpha * proj[rows:, half:]
    scaled_grad = jnp.zeros((rows, half), jnp.float32)
    later = jnp.zeros((rows, half), jnp.float32)
    weights = [None] * sections
    zero = jnp.zeros((rows, 1), jnp.float32)
    beta = zero
    for s in reversed(range(sections)):
        lowgrad = jnp.where(blocks[s], kept[s] * carried, 0.0).astype(jnp.bfloat16)
        lowgrad_f32 = lowgrad.astype(jnp.float32)
        mean = jnp.sum(lowgrad_f32 * down_saved, axis=1, keepdims=True) / width
        inverse = inverses[s]
        pull = inverse * inverse * inverse * mean
        weights[s] = pull
        scaled = inverse * lowgrad_f32
        scaled_grad += scaled
        if s > 0:
            back = lax.dot_general(
                lowgrad, gram_hi[:, :half], (((1,), (1,)), ((), ())), preferred_element_type=jnp.float32
            ) + lax.dot_general(
                lowgrad, gram_lo[:, :half], (((1,), (1,)), ((), ())), preferred_element_type=jnp.float32
            )
            carried = carried + inverse * back - pull * branch_stash[s]

    beta = zero
    gamma = jnp.zeros((rows, half), jnp.float32)
    for s in reversed(range(sections)):
        gamma = jnp.where(blocks[s], beta, gamma)
        beta = beta + jnp.where(s > own, weights[s], zero)
    low_edge = own * rank
    high_edge = low_edge + rank
    after = jnp.where(lane_ids >= high_edge, scaled_grad, 0.0).astype(jnp.bfloat16)
    before = jnp.where(lane_ids < low_edge, kept_low, 0.0).astype(jnp.bfloat16)
    pulled = (gamma * kept_low).astype(jnp.bfloat16)
    turned[0] = (alpha * kept_low).T
    turned[1] = (-beta * kept_low).T
    turned[2] = kept_low.T
    turned[3] = scaled_grad.T
    mine = pl.ds(pl.multiple_of(low_edge, 16), rank)
    low_own = turned[2, mine, :].astype(jnp.bfloat16)
    grad_own = turned[3, mine, :].astype(jnp.bfloat16)
    coef_up = [
        turned[1, mine, :].astype(jnp.bfloat16),
        turned[0, mine, :].astype(jnp.bfloat16),
        jnp.dot(low_own, after, preferred_element_type=jnp.float32).astype(jnp.bfloat16),
        -jnp.dot(low_own, pulled, preferred_element_type=jnp.float32).astype(jnp.bfloat16),
    ]
    coef_gain = [
        grad_own,
        jnp.dot(grad_own, before, preferred_element_type=jnp.float32).astype(jnp.bfloat16),
    ]
    left = jnp.concatenate(
        [
            jnp.concatenate([coef_up[2], coef_up[3], coef_up[0], coef_up[1]], axis=1),
            jnp.concatenate(
                [
                    jnp.zeros((rank, half), jnp.bfloat16),
                    coef_gain[1],
                    coef_gain[0],
                    jnp.zeros((rank, rows), jnp.bfloat16),
                ],
                axis=1,
            ),
        ],
        axis=0,
    )
    down_copy.wait()
    chunk = model_width // parts
    lane_blocks = chunk // LANES
    tail = payload_refs[0].shape[0] - lane_blocks * rank
    for k in range(parts):
        columns = pl.ds(pl.multiple_of((place ^ k) * chunk, LANES), chunk)
        result = jnp.dot(left, stack[:, columns], preferred_element_type=jnp.float32)
        gain = jnp.sum(
            result[rank:] * down[:, columns].astype(jnp.float32), axis=0, keepdims=True
        )
        for j in range(lane_blocks):
            payload_refs[k][j * rank : (j + 1) * rank, :] = result[
                :rank, j * LANES : (j + 1) * LANES
            ].astype(jnp.bfloat16)
        gain_rows = [gain[:, j * LANES : (j + 1) * LANES] for j in range(lane_blocks)]
        gain_rows.append(jnp.zeros((tail - lane_blocks, LANES), jnp.float32))
        payload_refs[k][lane_blocks * rank :, :] = jnp.concatenate(gain_rows, axis=0).astype(
            jnp.bfloat16
        )


def unpack_kernel(index_ref, *refs):
    parts_refs, (up_ref, gain_ref) = refs[:-2], refs[-2:]
    parts = len(parts_refs)
    rank = up_ref.shape[0]
    chunk = up_ref.shape[1] // parts
    lane_blocks = chunk // LANES
    for k in range(parts):
        start = (index_ref[2] ^ k) * chunk
        tail = parts_refs[k][lane_blocks * rank :, :].astype(jnp.float32)
        for j in range(lane_blocks):
            lanes = pl.ds(pl.multiple_of(start + j * LANES, LANES), LANES)
            up_ref[:, lanes] = parts_refs[k][j * rank : (j + 1) * rank, :].astype(jnp.float32)
            gain_ref[:, lanes] = tail[j : j + 1, :]


def summed(first, *others):
    total = first.astype(jnp.float32)
    for other in others:
        total = total + other.astype(jnp.float32)
    return total.astype(jnp.bfloat16)


def scattered_sum(blocks):
    parts = len(blocks)
    if parts == 1:
        return blocks[0]
    merged = {}
    for k in reversed(range(0, parts, 2)):
        merged[k] = summed(blocks[k], swapped(blocks[k + 1], "dp", 1))
    return summed(merged[0], *[swapped(merged[k], "dp", k) for k in reversed(range(2, parts, 2))])


def gathered_blocks(block):
    parts = lax.axis_size("dp")
    blocks = [block]
    if parts > 1:
        even = [block] + [swapped(block, "dp", k) for k in range(2, parts, 2)]
        blocks = [piece for one in even for piece in (one, swapped(one, "dp", 1))]
    return blocks


def rank_space_body(
    entry_tokens,
    section_norm_gain,
    adapter_down_weight,
    adapter_up_weight,
    output_gradient,
    lengths,
    keep,
):
    sections = lax.axis_size("section")
    parts = lax.axis_size("dp")
    section_index = lax.axis_index("section")
    micro, tokens, width = entry_tokens.shape[1:]
    rank = adapter_down_weight.shape[1]
    rows = micro * tokens
    down = adapter_down_weight[0]
    up = adapter_up_weight[0]
    place = lax.axis_index("dp")
    side = place & 1
    piece = width // PIECES
    edge = EDGE * piece
    near = side * (width - edge)
    up_edge = lax.dynamic_slice(up, (0, near), (rank, edge))
    scaled_down = (
        section_norm_gain[0].astype(jnp.float32) * down.astype(jnp.float32)
    ).astype(jnp.bfloat16)
    down_edge = lax.dynamic_slice(scaled_down, (0, near), (rank, edge))
    weights = jnp.concatenate([scaled_down, up], axis=0)
    middle = weights[:, edge : width - edge]
    valid = (jnp.arange(tokens, dtype=jnp.int32)[None, :] < lengths[0][:, None]).astype(jnp.float32)
    kept_all = lax.all_gather(keep[0, 0], "section").astype(jnp.float32) * valid[None]
    masks = jnp.concatenate([kept_all.reshape(sections, rows), valid.reshape(1, rows)], axis=0).T
    middle, masks = lax.optimization_barrier((middle, masks))
    regions = [
        ("tokens", 0, PIECES, True),
        ("grads", 0, PIECES, True),
        ((0, (0, 1)), 0, PIECES, True),
    ]
    sources = [entry_tokens.reshape(rows, width), output_gradient.reshape(rows, width), weights]
    if sections > 1:
        regions.append(((1, (0, 1)), 0, PIECES, True))
        sources.append(swapped(weights, "section", 1))
    for k in range(2, sections, 2):
        up_near = swapped(up_edge, "section", k)
        down_near = swapped(down_edge, "section", k)
        centre = swapped(middle, "section", k)
        up_away = swapped(up_near, "dp", 1)
        down_away = swapped(down_near, "dp", 1)
        arrived = [up_near, down_near, centre, up_away, down_away]
        arrived += [swapped(block, "section", 1) for block in arrived]
        for j in range(2):
            regions += [
                ((k + j, (1,)), 0, EDGE, False),
                ((k + j, (0,)), 0, EDGE, False),
                ((k + j, (0, 1)), EDGE, PIECES - EDGE, False),
                ((k + j, (1,)), PIECES - EDGE, PIECES, False),
                ((k + j, (0,)), PIECES - EDGE, PIECES, False),
            ]
        sources += arrived
    half = -(-sections * rank // LANES) * LANES
    lane_blocks = width // parts // LANES
    payload_rows = lane_blocks * rank + -(-lane_blocks // 16) * 16
    index = jnp.stack([section_index, side, place]).astype(jnp.int32)
    hbm = pl.BlockSpec(memory_space=pltpu.MemorySpace.HBM)
    vmem = pl.BlockSpec(memory_space=pltpu.MemorySpace.VMEM)
    smem = pl.BlockSpec(memory_space=pltpu.MemorySpace.SMEM)
    payload = pl.pallas_call(
        lambda *refs: rank_space_kernel(
            *refs,
            regions=regions,
            sections=sections,
            rank=rank,
            width=width,
            micro=micro,
            tokens=tokens,
            parts=parts,
        ),
        out_shape=[jax.ShapeDtypeStruct((payload_rows, LANES), jnp.bfloat16)] * parts,
        in_specs=[smem, vmem] + [hbm] * (len(sources) + 1),
        out_specs=[vmem] * parts,
        scratch_shapes=[
            pltpu.VMEM((2 * half + 2 * rows, width), jnp.bfloat16),
            pltpu.VMEM((rank, width), jnp.bfloat16),
            pltpu.VMEM((half, 2 * half), jnp.float32),
            pltpu.VMEM((2 * rows, 2 * half), jnp.float32),
            pltpu.VMEM((sections, rows, half), jnp.float32),
            pltpu.VMEM((4, half, rows), jnp.float32),
            pltpu.SemaphoreType.DMA((PIECES, 2 + 2 * sections)),
            pltpu.SemaphoreType.DMA(()),
        ],
        compiler_params=pltpu.CompilerParams(vmem_limit_bytes=VMEM_BUDGET),
        name="rank_space",
    )(index, masks, *sources, down)
    blocks = gathered_blocks(scattered_sum(payload))
    grad_up, grad_gain = pl.pallas_call(
        unpack_kernel,
        out_shape=(
            jax.ShapeDtypeStruct((rank, width), jnp.float32),
            jax.ShapeDtypeStruct((1, width), jnp.float32),
        ),
        in_specs=[smem] + [vmem] * parts,
        out_specs=(vmem, vmem),
        name="unpack",
    )(index, *blocks)
    return (grad_up[None], grad_gain)


def fits_rank_space(args, sections, parts):
    micro, tokens, width = args[0].shape[1:]
    rank = args[2].shape[1]
    rows = micro * tokens
    half = -(-sections * rank // LANES) * LANES
    return (
        sections & (sections - 1) == 0
        and parts & (parts - 1) == 0
        and width % (parts * LANES) == 0
        and width % (PIECES * LANES) == 0
        and rank % 16 == 0
        and rows % LANES == 0
        and tokens % 8 == 0
        and (2 * half + 2 * rows) * width * 2 <= VMEM_BUDGET // 3
    )


def body(*args):
    if fits_rank_space(args, lax.axis_size("section"), lax.axis_size("dp")):
        return rank_space_body(*args)
    return relay_body(*args)


def solution(mesh):
    in_specs = (
        P("dp", None, None, None),
        P("section", None),
        P("section", None, None),
        P("section", None, None),
        P("dp", None, None, None),
        P("dp", None),
        P("dp", "section", None, None),
    )
    out_specs = (P("section", None, None), P("section", None))
    return jax.shard_map(body, mesh=mesh, in_specs=in_specs, out_specs=out_specs, check_vma=False)
```

```python
import jax
import jax.numpy as jnp
from jax import lax
from jax.experimental import pallas as pl
from jax.experimental.pallas import tpu as pltpu
from jax.sharding import PartitionSpec as P

EPS = 1e-05


def passed_along(block, axis, distance):
    devices = range(lax.axis_size(axis))
    route = [(i - distance, i) for i in devices if i - distance in devices]
    return lax.ppermute(block, axis, route)


def section_apply(current_rows, gain_f32, down_rows, up_rows, weight):
    widened_rows = current_rows.astype(jnp.float32)
    inverse_norm = lax.rsqrt(jnp.mean(widened_rows * widened_rows, axis=-1, keepdims=True) + EPS)
    normed = (widened_rows * inverse_norm * gain_f32).astype(jnp.bfloat16)
    lowrank_rows = lax.dot_general(
        normed, down_rows, (((1,), (1,)), ((), ())), preferred_element_type=jnp.float32
    ).astype(jnp.bfloat16)
    branch = jnp.dot(lowrank_rows, up_rows, preferred_element_type=jnp.float32)
    section_output = (widened_rows + weight * branch).astype(jnp.bfloat16)
    row_energy = jnp.sum(weight * branch * branch, axis=1)
    return (section_output, lowrank_rows, row_energy)


def relay_body(
    entry_tokens,
    section_norm_gain,
    adapter_down_weight,
    adapter_up_weight,
    output_gradient,
    lengths,
    keep,
):
    section_total = lax.axis_size("section")
    section_index = lax.axis_index("section")
    micro_count = entry_tokens.shape[1]
    token_count = entry_tokens.shape[2]
    model_width = entry_tokens.shape[3]
    rank_total = adapter_down_weight.shape[1]
    group_size = 2
    block_count = micro_count // group_size
    block_rows = group_size * token_count
    gain_f32 = section_norm_gain[0].astype(jnp.float32)
    down_rows = adapter_down_weight[0]
    up_rows = adapter_up_weight[0]
    position = jnp.arange(token_count, dtype=jnp.int32)
    valid_mask = (position[None, :] < lengths[0][:, None]).astype(jnp.float32)
    retained_mask = keep[0, 0].astype(jnp.float32) * valid_mask
    count_local = jnp.sum(retained_mask, axis=1)
    tick_count = block_count + section_total - 1
    block_ids = jnp.arange(block_count, dtype=jnp.int32)
    tokens_blocks = entry_tokens[0].reshape(block_count, block_rows, model_width)
    grad_blocks = output_gradient[0].reshape(block_count, block_rows, model_width)
    kept_blocks = retained_mask.reshape(block_count, block_rows)
    valid_blocks = valid_mask.reshape(block_count, block_rows)

    def forward_tick(step_index, state_tuple):
        incoming, stashed, low_stash, energy = state_tuple
        block_index = step_index - section_index
        active = (block_index >= 0) & (block_index < block_count)
        slot_index = jnp.clip(block_index, 0, block_count - 1)
        fresh_rows = lax.dynamic_index_in_dim(tokens_blocks, slot_index, 0, keepdims=False)
        current_rows = jnp.where(section_index == 0, fresh_rows, incoming)
        weight = lax.dynamic_index_in_dim(kept_blocks, slot_index, 0, keepdims=False)[:, None]
        section_output, lowrank_rows, row_energy = section_apply(
            current_rows, gain_f32, down_rows, up_rows, weight
        )
        block_energy = jnp.sum(row_energy.reshape(group_size, token_count), axis=1)
        old_rows = lax.dynamic_index_in_dim(stashed, slot_index, 0, keepdims=False)
        stashed = lax.dynamic_update_index_in_dim(
            stashed, jnp.where(active, current_rows, old_rows), slot_index, 0
        )
        old_low = lax.dynamic_index_in_dim(low_stash, slot_index, 0, keepdims=False)
        low_stash = lax.dynamic_update_index_in_dim(
            low_stash, jnp.where(active, lowrank_rows, old_low), slot_index, 0
        )
        energy = (
            energy + (block_ids == block_index).astype(jnp.float32)[:, None] * block_energy[None, :]
        )
        passed = passed_along(section_output, "section", 1)
        return (passed, stashed, low_stash, energy)

    start_state = (
        jnp.zeros((block_rows, model_width), jnp.bfloat16),
        jnp.zeros((block_count, block_rows, model_width), jnp.bfloat16),
        jnp.zeros((block_count, block_rows, rank_total), jnp.bfloat16),
        jnp.zeros((block_count, group_size), jnp.float32),
    )
    ignored, stashed, low_stash, energy_blocks = lax.fori_loop(
        0, tick_count, forward_tick, start_state
    )
    energy = energy_blocks.reshape(micro_count)
    total_energy, total_count = lax.psum((energy, count_local), "section")
    scaling = 1.0 / (total_count * jnp.sqrt(total_energy / (model_width * total_count) + EPS))
    scaling_rows = (scaling[:, None] * jnp.ones((1, token_count), jnp.float32)).reshape(
        block_count, block_rows
    )

    def backward_tick(step_index, state_tuple):
        incoming, grad_stash, gain_grad = state_tuple
        block_index = step_index - (section_total - 1 - section_index)
        active = (block_index >= 0) & (block_index < block_count)
        slot_index = jnp.clip(block_index, 0, block_count - 1)
        valid_row = lax.dynamic_index_in_dim(valid_blocks, slot_index, 0, keepdims=False)[:, None]
        scale_row = lax.dynamic_index_in_dim(scaling_rows, slot_index, 0, keepdims=False)[:, None]
        seed_rows = (
            lax.dynamic_index_in_dim(grad_blocks, slot_index, 0, keepdims=False).astype(jnp.float32)
            * valid_row
            * scale_row
        ).astype(jnp.bfloat16)
        cotangent = jnp.where(section_index == section_total - 1, seed_rows, incoming)
        current_rows = lax.dynamic_index_in_dim(stashed, slot_index, 0, keepdims=False)
        weight = lax.dynamic_index_in_dim(kept_blocks, slot_index, 0, keepdims=False)[:, None]
        widened_rows = current_rows.astype(jnp.float32)
        inverse_norm = lax.rsqrt(
            jnp.mean(widened_rows * widened_rows, axis=-1, keepdims=True) + EPS
        )
        branch_gradient = (weight * cotangent.astype(jnp.float32)).astype(jnp.bfloat16)
        lowrank_gradient = lax.dot_general(
            branch_gradient, up_rows, (((1,), (1,)), ((), ())), preferred_element_type=jnp.float32
        ).astype(jnp.bfloat16)
        norm_gradient = jnp.dot(lowrank_gradient, down_rows, preferred_element_type=jnp.float32)
        gain_grad = gain_grad + jnp.where(
            active, jnp.sum(norm_gradient * widened_rows * inverse_norm, axis=0), 0.0
        )
        scaled = norm_gradient * gain_f32
        input_grad = inverse_norm * scaled - widened_rows * inverse_norm**3 * jnp.mean(
            scaled * widened_rows, axis=-1, keepdims=True
        )
        updated = (cotangent.astype(jnp.float32) + input_grad).astype(jnp.bfloat16)
        old_rows = lax.dynamic_index_in_dim(grad_stash, slot_index, 0, keepdims=False)
        grad_stash = lax.dynamic_update_index_in_dim(
            grad_stash, jnp.where(active, branch_gradient, old_rows), slot_index, 0
        )
        passed = passed_along(updated, "section", -1)
        return (passed, grad_stash, gain_grad)

    back_state = (
        jnp.zeros((block_rows, model_width), jnp.bfloat16),
        jnp.zeros((block_count, block_rows, model_width), jnp.bfloat16),
        jnp.zeros((model_width,), jnp.float32),
    )
    ignored, grad_stash, gain_grad = lax.fori_loop(0, tick_count, backward_tick, back_state)
    low_rows = low_stash.reshape(micro_count * token_count, rank_total)
    grad_rows = grad_stash.reshape(micro_count * token_count, model_width)
    grad_section = lax.dot_general(
        low_rows, grad_rows, (((0,), (0,)), ((), ())), preferred_element_type=jnp.float32
    )
    summed_up, summed_gain = lax.psum((grad_section, gain_grad), "dp")
    return (summed_up[None], summed_gain[None])


LANES = 128
PIECES = 8
EDGE = 3
PAIR = 2
VMEM_BUDGET = 24 * 1024 * 1024


def swapped(block, axis, bit):
    route = [(i, i ^ bit) for i in range(lax.axis_size(axis))]
    return lax.ppermute(block, axis, route)


def pair_rows(rel, rank):
    return (rel // PAIR) * LANES + (rel % PAIR) * rank


def near_kernel(tokens_hbm, grads_hbm, own_hbm, other_hbm, stack, gram_ref, kept_ref, sems):
    rows = tokens_hbm.shape[0]
    rank = own_hbm.shape[0] // 2
    model_width = tokens_hbm.shape[1]
    piece = model_width // PIECES
    copies = []
    for p in range(PIECES):
        columns = pl.ds(p * piece, piece)
        moves = [(tokens_hbm, 0, 2 * LANES, rows), (grads_hbm, 0, 2 * LANES + rows, rows)]
        for j, source in enumerate((own_hbm, other_hbm)):
            for q in range(2):
                moves.append((source, q * rank, q * LANES + j * rank, rank))
        group = [
            pltpu.make_async_copy(
                source.at[pl.ds(from_row, count), columns],
                stack.at[pl.ds(to_row, count), columns],
                sems.at[p, i],
            )
            for i, (source, from_row, to_row, count) in enumerate(moves)
        ]
        for copy in group:
            copy.start()
        copies.append(group)
    flags = [
        pltpu.make_async_copy(
            source.at[pl.ds(0, 16), pl.ds(model_width, LANES)], kept_ref.at[j], sems.at[j, 6]
        )
        for j, source in enumerate((own_hbm, other_hbm))
    ]
    for copy in flags:
        copy.start()
    top = 2 * LANES + 2 * rows
    for base in (0, LANES, top, top + LANES):
        stack[base + PAIR * rank : base + LANES, :] = jnp.zeros(
            (LANES - PAIR * rank, model_width), jnp.bfloat16
        )
    joined = 2
    for p in range(0, PIECES, joined):
        for group in copies[p : p + joined]:
            for copy in group:
                copy.wait()
        columns = slice(p * piece, (p + joined) * piece)
        product = lax.dot_general(
            stack[LANES:top, columns],
            stack[: 2 * LANES, columns],
            (((1,), (1,)), ((), ())),
            preferred_element_type=jnp.float32,
        )
        if p == 0:
            gram_ref[: top - LANES, :] = product
            square = jnp.zeros((rows, LANES), jnp.float32)
        else:
            gram_ref[: top - LANES, :] += product
        values = stack[2 * LANES : 2 * LANES + rows, columns].astype(jnp.float32)
        for j in range(joined * piece // LANES):
            part = values[:, j * LANES : (j + 1) * LANES]
            square += part * part
    gram_ref[top - LANES :, :LANES] = square
    gram_ref[top - LANES :, LANES:] = jnp.zeros((rows, LANES), jnp.float32)
    for copy in flags:
        copy.wait()


def rank_space_kernel(
    index_ref, valid_ref, near_gram_ref, near_kept_ref, *rest, regions, sections, rank, width,
    micro, tokens, parts
):
    sources = rest[: len(regions)]
    down, stack_in = rest[len(regions) : len(regions) + 2]
    payload_refs = rest[len(regions) + 2 : len(regions) + 2 + parts]
    stack, gram, proj, branch_stash = rest[len(regions) + 2 + parts :]
    del stack_in
    rows = micro * tokens
    half = 2 * LANES
    top = half + 2 * rows
    model_width = stack.shape[1]
    piece = model_width // PIECES
    own = index_ref[0]
    side = index_ref[1]
    place = index_ref[2]
    near = pl.multiple_of(side * (PIECES - EDGE) * piece, LANES)
    away = pl.multiple_of((1 - side) * (PIECES - EDGE) * piece, LANES)
    offsets = {"near": near, "away": away, "middle": EDGE * piece}
    for source, (rel, matrices, where) in zip(sources, regions):
        lanes = (PIECES - 2 * EDGE if where == "middle" else EDGE) * piece
        for i, q in enumerate(matrices):
            base = top + (1 - q) * LANES + (rel % PAIR) * rank
            stack[base : base + rank, pl.ds(offsets[where], lanes)] = source[
                i * rank : (i + 1) * rank, :lanes
            ]
    joined = model_width // 2
    for p in range(2):
        columns = slice(p * joined, (p + 1) * joined)
        product = lax.dot_general(
            stack[: top + LANES, columns],
            stack[top:, columns],
            (((1,), (1,)), ((), ())),
            preferred_element_type=jnp.float32,
        )
        if p == 0:
            proj[...] = product
        else:
            proj[...] += product
    down_near, down_far, up_near, up_far = [slice(i * LANES, (i + 1) * LANES) for i in range(4)]
    far_up, far_down = slice(0, LANES), slice(LANES, half)
    gram[:LANES, down_near] = near_gram_ref[:LANES, :LANES]
    gram[:LANES, up_near] = near_gram_ref[:LANES, LANES:]
    gram[:LANES, up_far] = proj[LANES:half, far_up]
    gram[:LANES, down_far] = proj[LANES:half, far_down]
    gram[LANES:, down_near] = proj[:LANES, far_up].T
    gram[LANES:, up_near] = proj[LANES:half, far_up].T
    gram[LANES:, up_far] = proj[top:, far_up]
    gram[LANES:, down_far] = proj[top:, far_down]
    norm_sq = jnp.sum(near_gram_ref[LANES + 2 * rows :, :LANES], axis=1, keepdims=True)
    token_near = near_gram_ref[LANES : LANES + rows, :]
    grad_near = near_gram_ref[LANES + rows : LANES + 2 * rows, :]
    token_far = proj[half : half + rows, :]
    grad_far = proj[half + rows : top, :]

    flag_rows = [near_kept_ref[j, 0:1, :].astype(jnp.float32) for j in range(PAIR)]
    for source, (rel, matrices, where) in zip(sources, regions):
        if where == "near" and matrices == (0,):
            flag_rows.append(source[0:16, EDGE * piece :].astype(jnp.float32)[0:1, :])
    ordered = []
    for s in range(sections):
        row = flag_rows[0]
        for j in range(1, sections):
            row = jnp.where((own ^ s) == j, flag_rows[j], row)
        ordered.append(row)
    ordered.append(valid_ref[...])
    ordered.append(jnp.zeros((LANES - len(ordered), rows), jnp.float32))
    masks = jnp.concatenate(ordered, axis=0).T
    lane_ids = lax.broadcasted_iota(jnp.int32, (rows, half), 1)
    firsts = [pair_rows(own ^ s, rank) for s in range(sections)]
    blocks = [(lane_ids >= first) & (lane_ids < first + rank) for first in firsts]
    kept = [masks[:, s : s + 1] for s in range(sections)]
    valid = masks[:, sections : sections + 1]
    gram_hi = gram[...].astype(jnp.bfloat16)
    gram_lo = (gram[...] - gram_hi.astype(jnp.float32)).astype(jnp.bfloat16)
    down_side = jnp.concatenate([token_near[:, :LANES], token_far[:, far_down]], axis=1)
    up_side = jnp.concatenate([token_near[:, LANES:], token_far[:, far_up]], axis=1)
    down_saved = jnp.zeros((rows, half), jnp.float32)
    kept_low = jnp.zeros((rows, half), jnp.float32)
    power = jnp.zeros((rows, 1), jnp.float32)
    count = jnp.zeros((rows, 1), jnp.float32)
    inverses = []
    for s in range(sections):
        inverse = lax.rsqrt(norm_sq / width + EPS)
        inverses.append(inverse)
        masked = jnp.where(blocks[s], down_side, 0.0)
        down_saved += masked
        low = (masked * inverse).astype(jnp.bfloat16)
        low_f32 = low.astype(jnp.float32)
        kept_low += kept[s] * low_f32
        branch_stash[s] = up_side
        moved = jnp.dot(low, gram_hi, preferred_element_type=jnp.float32) + jnp.dot(
            low, gram_lo, preferred_element_type=jnp.float32
        )
        energy = jnp.sum(low_f32 * moved[:, half:], axis=1, keepdims=True)
        cross = jnp.sum(low_f32 * up_side, axis=1, keepdims=True)
        power += kept[s] * energy
        count += kept[s]
        norm_sq = jnp.maximum(norm_sq + kept[s] * (2.0 * cross + energy), 0.0)
        down_side = down_side + kept[s] * moved[:, :half]
        up_side = up_side + kept[s] * moved[:, half:]

    def per_micro(column):
        wide = jnp.broadcast_to(column, (rows, LANES)).reshape(micro, tokens, LANES)
        total = jnp.broadcast_to(jnp.sum(wide, axis=1, keepdims=True), wide.shape)
        return total.reshape(rows, LANES)[:, :1]

    total_energy = jnp.maximum(per_micro(power), 0.0)
    total_count = per_micro(count)
    scaling = 1.0 / (total_count * jnp.sqrt(total_energy / (width * total_count) + EPS))
    alpha = valid * scaling

    carried = alpha * jnp.concatenate([grad_near[:, LANES:], grad_far[:, far_up]], axis=1)
    scaled_grad = jnp.zeros((rows, half), jnp.float32)
    later = jnp.zeros((rows, half), jnp.float32)
    weights = [None] * sections
    zero = jnp.zeros((rows, 1), jnp.float32)
    beta = zero
    for s in reversed(range(sections)):
        lowgrad = jnp.where(blocks[s], kept[s] * carried, 0.0).astype(jnp.bfloat16)
        lowgrad_f32 = lowgrad.astype(jnp.float32)
        mean = jnp.sum(lowgrad_f32 * down_saved, axis=1, keepdims=True) / width
        inverse = inverses[s]
        pull = inverse * inverse * inverse * mean
        weights[s] = pull
        scaled = inverse * lowgrad_f32
        scaled_grad += scaled
        if s > 0:
            back = lax.dot_general(
                lowgrad, gram_hi[:, :half], (((1,), (1,)), ((), ())), preferred_element_type=jnp.float32
            ) + lax.dot_general(
                lowgrad, gram_lo[:, :half], (((1,), (1,)), ((), ())), preferred_element_type=jnp.float32
            )
            carried = carried + inverse * back - pull * branch_stash[s]

    beta = zero
    gamma = jnp.zeros((rows, half), jnp.float32)
    after = jnp.zeros((rows, half), jnp.float32)
    before = jnp.zeros((rows, half), jnp.float32)
    for s in reversed(range(sections)):
        gamma = jnp.where(blocks[s], beta, gamma)
        beta = beta + jnp.where(s > own, weights[s], zero)
        after = jnp.where(blocks[s] & (s > own), scaled_grad, after)
        before = jnp.where(blocks[s] & (s < own), kept_low, before)
    after = after.astype(jnp.bfloat16)
    before = before.astype(jnp.bfloat16)
    pulled = (gamma * kept_low).astype(jnp.bfloat16)
    low_part = kept_low[:, :LANES]
    low_own = low_part.T[:rank].astype(jnp.bfloat16)
    grad_own = scaled_grad[:, :LANES].T[:rank].astype(jnp.bfloat16)
    from_grads = (alpha * low_part).T[:rank].astype(jnp.bfloat16)
    from_tokens = (-beta * low_part).T[:rank].astype(jnp.bfloat16)
    from_down = jnp.dot(low_own, after, preferred_element_type=jnp.float32).astype(jnp.bfloat16)
    from_up = -jnp.dot(low_own, pulled, preferred_element_type=jnp.float32).astype(jnp.bfloat16)
    gain_up = jnp.dot(grad_own, before, preferred_element_type=jnp.float32).astype(jnp.bfloat16)
    blank = jnp.zeros((rank, LANES), jnp.bfloat16)
    left = jnp.concatenate(
        [
            jnp.concatenate(
                [
                    from_down[:, :LANES], from_up[:, :LANES], from_tokens, from_grads,
                    from_up[:, LANES:], from_down[:, LANES:],
                ],
                axis=1,
            ),
            jnp.concatenate(
                [blank, gain_up[:, :LANES], grad_own, blank, gain_up[:, LANES:], blank], axis=1
            ),
        ],
        axis=0,
    )
    chunk = model_width // parts
    lane_blocks = chunk // LANES
    tail = payload_refs[0].shape[0] - lane_blocks * rank
    for k in range(parts):
        columns = pl.ds(pl.multiple_of((place ^ k) * chunk, LANES), chunk)
        result = jnp.dot(left, stack[:, columns], preferred_element_type=jnp.float32)
        gain = jnp.sum(
            result[rank:] * down[:, columns].astype(jnp.float32), axis=0, keepdims=True
        )
        for j in range(lane_blocks):
            payload_refs[k][j * rank : (j + 1) * rank, :] = result[
                :rank, j * LANES : (j + 1) * LANES
            ].astype(jnp.bfloat16)
        gain_rows = [gain[:, j * LANES : (j + 1) * LANES] for j in range(lane_blocks)]
        gain_rows.append(jnp.zeros((tail - lane_blocks, LANES), jnp.float32))
        payload_refs[k][lane_blocks * rank :, :] = jnp.concatenate(gain_rows, axis=0).astype(
            jnp.bfloat16
        )


def unpack_kernel(index_ref, *refs):
    parts_refs, (up_ref, gain_ref) = refs[:-2], refs[-2:]
    parts = len(parts_refs)
    rank = up_ref.shape[0]
    chunk = up_ref.shape[1] // parts
    lane_blocks = chunk // LANES
    for k in range(parts):
        start = (index_ref[2] ^ k) * chunk
        tail = parts_refs[k][lane_blocks * rank :, :].astype(jnp.float32)
        for j in range(lane_blocks):
            lanes = pl.ds(pl.multiple_of(start + j * LANES, LANES), LANES)
            up_ref[:, lanes] = parts_refs[k][j * rank : (j + 1) * rank, :].astype(jnp.float32)
            gain_ref[:, lanes] = tail[j : j + 1, :]


def summed(first, *others):
    total = first.astype(jnp.float32)
    for other in others:
        total = total + other.astype(jnp.float32)
    return total.astype(jnp.bfloat16)


def scattered_sum(blocks):
    parts = len(blocks)
    if parts == 1:
        return blocks[0]
    merged = {}
    for k in reversed(range(0, parts, 2)):
        merged[k] = summed(blocks[k], swapped(blocks[k + 1], "dp", 1))
    return summed(merged[0], *[swapped(merged[k], "dp", k) for k in reversed(range(2, parts, 2))])


def gathered_blocks(block):
    parts = lax.axis_size("dp")
    blocks = [block]
    if parts > 1:
        even = [block] + [swapped(block, "dp", k) for k in range(2, parts, 2)]
        blocks = [piece for one in even for piece in (one, swapped(one, "dp", 1))]
    return blocks


def rank_space_body(
    entry_tokens,
    section_norm_gain,
    adapter_down_weight,
    adapter_up_weight,
    output_gradient,
    lengths,
    keep,
):
    sections = lax.axis_size("section")
    parts = lax.axis_size("dp")
    section_index = lax.axis_index("section")
    micro, tokens, width = entry_tokens.shape[1:]
    rank = adapter_down_weight.shape[1]
    rows = micro * tokens
    down = adapter_down_weight[0]
    up = adapter_up_weight[0]
    place = lax.axis_index("dp")
    side = place & 1
    piece = width // PIECES
    edge = EDGE * piece
    near = side * (width - edge)
    up_edge = lax.dynamic_slice(up, (0, near), (rank, edge))
    valid = (jnp.arange(tokens, dtype=jnp.int32)[None, :] < lengths[0][:, None]).astype(jnp.float32)
    kept = (keep[0, 0].astype(jnp.float32) * valid).reshape(1, rows)
    flags = jnp.pad(kept.astype(jnp.bfloat16), ((0, rank - 1), (0, 0)))
    scaled_down = (
        section_norm_gain[0].astype(jnp.float32) * down.astype(jnp.float32)
    ).astype(jnp.bfloat16)
    down_edge = jnp.concatenate(
        [lax.dynamic_slice(scaled_down, (0, near), (rank, edge)), flags], axis=1
    )
    weights = jnp.concatenate(
        [
            jnp.concatenate([scaled_down, flags], axis=1),
            jnp.pad(up, ((0, 0), (0, LANES))),
        ],
        axis=0,
    )
    middle = jnp.concatenate(
        [scaled_down[:, edge : width - edge], up[:, edge : width - edge]], axis=0
    )
    hbm = pl.BlockSpec(memory_space=pltpu.MemorySpace.HBM)
    vmem = pl.BlockSpec(memory_space=pltpu.MemorySpace.VMEM)
    smem = pl.BlockSpec(memory_space=pltpu.MemorySpace.SMEM)

    def on_chip(block):
        return pltpu.with_memory_space_constraint(block, pltpu.MemorySpace.VMEM)

    up_near = swapped(up_edge, "section", PAIR)
    down_near = swapped(down_edge, "section", PAIR)
    beside = swapped(weights, "section", 1)
    centre = swapped(middle, "section", PAIR)
    up_near, beside = lax.optimization_barrier((up_near, beside))
    stack_rows = 4 * LANES + 2 * rows
    stack, near_gram, near_kept = pl.pallas_call(
        near_kernel,
        out_shape=(
            pltpu.VMEM((stack_rows, width), jnp.bfloat16),
            pltpu.VMEM((LANES + 3 * rows, 2 * LANES), jnp.float32),
            pltpu.VMEM((PAIR, 16, LANES), jnp.bfloat16),
        ),
        in_specs=[hbm] * 4,
        out_specs=(vmem, vmem, vmem),
        scratch_shapes=[pltpu.SemaphoreType.DMA((PIECES, 7))],
        compiler_params=pltpu.CompilerParams(vmem_limit_bytes=VMEM_BUDGET),
        name="near_weights",
    )(
        entry_tokens.reshape(rows, width),
        output_gradient.reshape(rows, width),
        weights,
        beside,
    )
    up_away = swapped(up_near, "dp", 1)
    down_away = swapped(down_near, "dp", 1)
    regions = []
    sources = []
    for j in range(PAIR):
        regions += [
            (PAIR + j, (1,), "near"),
            (PAIR + j, (0,), "near"),
            (PAIR + j, (0, 1), "middle"),
            (PAIR + j, (1,), "away"),
            (PAIR + j, (0,), "away"),
        ]
    sources = [up_near, down_near, centre, up_away, down_away]
    sources += [swapped(block, "section", 1) for block in sources]
    lane_blocks = width // parts // LANES
    payload_rows = lane_blocks * rank + -(-lane_blocks // 16) * 16
    index = jnp.stack([section_index, side, place]).astype(jnp.int32)
    *payload, _ = pl.pallas_call(
        lambda *refs: rank_space_kernel(
            *refs,
            regions=regions,
            sections=sections,
            rank=rank,
            width=width,
            micro=micro,
            tokens=tokens,
            parts=parts,
        ),
        out_shape=[pltpu.VMEM((payload_rows, LANES), jnp.bfloat16)] * parts
        + [pltpu.VMEM((stack_rows, width), jnp.bfloat16)],
        in_specs=[smem] + [vmem] * (len(sources) + 5),
        out_specs=[vmem] * (parts + 1),
        input_output_aliases={len(sources) + 5: parts},
        scratch_shapes=[
            pltpu.VMEM((2 * LANES, 4 * LANES), jnp.float32),
            pltpu.VMEM((3 * LANES + 2 * rows, 2 * LANES), jnp.float32),
            pltpu.VMEM((sections, rows, 2 * LANES), jnp.float32),
        ],
        compiler_params=pltpu.CompilerParams(vmem_limit_bytes=VMEM_BUDGET),
        name="rank_space",
    )(
        index,
        valid.reshape(1, rows),
        near_gram,
        near_kept,
        *[on_chip(block) for block in sources],
        on_chip(down),
        stack,
    )
    blocks = gathered_blocks(scattered_sum(payload))
    grad_up, grad_gain = pl.pallas_call(
        unpack_kernel,
        out_shape=(
            jax.ShapeDtypeStruct((rank, width), jnp.float32),
            jax.ShapeDtypeStruct((1, width), jnp.float32),
        ),
        in_specs=[smem] + [vmem] * parts,
        out_specs=(vmem, vmem),
        name="unpack",
    )(index, *[on_chip(block) for block in blocks])
    return (grad_up[None], grad_gain)


def fits_rank_space(args, sections, parts):
    micro, tokens, width = args[0].shape[1:]
    rank = args[2].shape[1]
    return (
        sections == 2 * PAIR
        and parts > 1
        and parts & (parts - 1) == 0
        and width % (parts * LANES) == 0
        and width % (PIECES * LANES) == 0
        and rank % 16 == 0
        and PAIR * rank <= LANES
        and micro * tokens == LANES
        and tokens % 8 == 0
        and 6 * LANES * width * 2 <= VMEM_BUDGET
    )


def body(*args):
    if fits_rank_space(args, lax.axis_size("section"), lax.axis_size("dp")):
        return rank_space_body(*args)
    return relay_body(*args)


def solution(mesh):
    in_specs = (
        P("dp", None, None, None),
        P("section", None),
        P("section", None, None),
        P("section", None, None),
        P("dp", None, None, None),
        P("dp", None),
        P("dp", "section", None, None),
    )
    out_specs = (P("section", None, None), P("section", None))
    return jax.shard_map(body, mesh=mesh, in_specs=in_specs, out_specs=out_specs, check_vma=False)
```

```python
import functools

import jax
import jax.numpy as jnp
from jax import lax
from jax.experimental import pallas as pl
from jax.experimental.pallas import tpu as pltpu
from jax.sharding import PartitionSpec as P

EPS = 1e-05


def passed_along(block, axis, distance):
    devices = range(lax.axis_size(axis))
    route = [(i - distance, i) for i in devices if i - distance in devices]
    return lax.ppermute(block, axis, route)


def section_apply(current_rows, gain_f32, down_rows, up_rows, weight):
    widened_rows = current_rows.astype(jnp.float32)
    inverse_norm = lax.rsqrt(jnp.mean(widened_rows * widened_rows, axis=-1, keepdims=True) + EPS)
    normed = (widened_rows * inverse_norm * gain_f32).astype(jnp.bfloat16)
    lowrank_rows = lax.dot_general(
        normed, down_rows, (((1,), (1,)), ((), ())), preferred_element_type=jnp.float32
    ).astype(jnp.bfloat16)
    branch = jnp.dot(lowrank_rows, up_rows, preferred_element_type=jnp.float32)
    section_output = (widened_rows + weight * branch).astype(jnp.bfloat16)
    row_energy = jnp.sum(weight * branch * branch, axis=1)
    return (section_output, lowrank_rows, row_energy)


def relay_body(
    entry_tokens,
    section_norm_gain,
    adapter_down_weight,
    adapter_up_weight,
    output_gradient,
    lengths,
    keep,
):
    section_total = lax.axis_size("section")
    section_index = lax.axis_index("section")
    micro_count = entry_tokens.shape[1]
    token_count = entry_tokens.shape[2]
    model_width = entry_tokens.shape[3]
    rank_total = adapter_down_weight.shape[1]
    group_size = 2
    block_count = micro_count // group_size
    block_rows = group_size * token_count
    gain_f32 = section_norm_gain[0].astype(jnp.float32)
    down_rows = adapter_down_weight[0]
    up_rows = adapter_up_weight[0]
    position = jnp.arange(token_count, dtype=jnp.int32)
    valid_mask = (position[None, :] < lengths[0][:, None]).astype(jnp.float32)
    retained_mask = keep[0, 0].astype(jnp.float32) * valid_mask
    count_local = jnp.sum(retained_mask, axis=1)
    tick_count = block_count + section_total - 1
    block_ids = jnp.arange(block_count, dtype=jnp.int32)
    tokens_blocks = entry_tokens[0].reshape(block_count, block_rows, model_width)
    grad_blocks = output_gradient[0].reshape(block_count, block_rows, model_width)
    kept_blocks = retained_mask.reshape(block_count, block_rows)
    valid_blocks = valid_mask.reshape(block_count, block_rows)

    def forward_tick(step_index, state_tuple):
        incoming, stashed, low_stash, energy = state_tuple
        block_index = step_index - section_index
        active = (block_index >= 0) & (block_index < block_count)
        slot_index = jnp.clip(block_index, 0, block_count - 1)
        fresh_rows = lax.dynamic_index_in_dim(tokens_blocks, slot_index, 0, keepdims=False)
        current_rows = jnp.where(section_index == 0, fresh_rows, incoming)
        weight = lax.dynamic_index_in_dim(kept_blocks, slot_index, 0, keepdims=False)[:, None]
        section_output, lowrank_rows, row_energy = section_apply(
            current_rows, gain_f32, down_rows, up_rows, weight
        )
        block_energy = jnp.sum(row_energy.reshape(group_size, token_count), axis=1)
        old_rows = lax.dynamic_index_in_dim(stashed, slot_index, 0, keepdims=False)
        stashed = lax.dynamic_update_index_in_dim(
            stashed, jnp.where(active, current_rows, old_rows), slot_index, 0
        )
        old_low = lax.dynamic_index_in_dim(low_stash, slot_index, 0, keepdims=False)
        low_stash = lax.dynamic_update_index_in_dim(
            low_stash, jnp.where(active, lowrank_rows, old_low), slot_index, 0
        )
        energy = (
            energy + (block_ids == block_index).astype(jnp.float32)[:, None] * block_energy[None, :]
        )
        passed = passed_along(section_output, "section", 1)
        return (passed, stashed, low_stash, energy)

    start_state = (
        jnp.zeros((block_rows, model_width), jnp.bfloat16),
        jnp.zeros((block_count, block_rows, model_width), jnp.bfloat16),
        jnp.zeros((block_count, block_rows, rank_total), jnp.bfloat16),
        jnp.zeros((block_count, group_size), jnp.float32),
    )
    ignored, stashed, low_stash, energy_blocks = lax.fori_loop(
        0, tick_count, forward_tick, start_state
    )
    energy = energy_blocks.reshape(micro_count)
    total_energy, total_count = lax.psum((energy, count_local), "section")
    scaling = 1.0 / (total_count * jnp.sqrt(total_energy / (model_width * total_count) + EPS))
    scaling_rows = (scaling[:, None] * jnp.ones((1, token_count), jnp.float32)).reshape(
        block_count, block_rows
    )

    def backward_tick(step_index, state_tuple):
        incoming, grad_stash, gain_grad = state_tuple
        block_index = step_index - (section_total - 1 - section_index)
        active = (block_index >= 0) & (block_index < block_count)
        slot_index = jnp.clip(block_index, 0, block_count - 1)
        valid_row = lax.dynamic_index_in_dim(valid_blocks, slot_index, 0, keepdims=False)[:, None]
        scale_row = lax.dynamic_index_in_dim(scaling_rows, slot_index, 0, keepdims=False)[:, None]
        seed_rows = (
            lax.dynamic_index_in_dim(grad_blocks, slot_index, 0, keepdims=False).astype(jnp.float32)
            * valid_row
            * scale_row
        ).astype(jnp.bfloat16)
        cotangent = jnp.where(section_index == section_total - 1, seed_rows, incoming)
        current_rows = lax.dynamic_index_in_dim(stashed, slot_index, 0, keepdims=False)
        weight = lax.dynamic_index_in_dim(kept_blocks, slot_index, 0, keepdims=False)[:, None]
        widened_rows = current_rows.astype(jnp.float32)
        inverse_norm = lax.rsqrt(
            jnp.mean(widened_rows * widened_rows, axis=-1, keepdims=True) + EPS
        )
        branch_gradient = (weight * cotangent.astype(jnp.float32)).astype(jnp.bfloat16)
        lowrank_gradient = lax.dot_general(
            branch_gradient, up_rows, (((1,), (1,)), ((), ())), preferred_element_type=jnp.float32
        ).astype(jnp.bfloat16)
        norm_gradient = jnp.dot(lowrank_gradient, down_rows, preferred_element_type=jnp.float32)
        gain_grad = gain_grad + jnp.where(
            active, jnp.sum(norm_gradient * widened_rows * inverse_norm, axis=0), 0.0
        )
        scaled = norm_gradient * gain_f32
        input_grad = inverse_norm * scaled - widened_rows * inverse_norm**3 * jnp.mean(
            scaled * widened_rows, axis=-1, keepdims=True
        )
        updated = (cotangent.astype(jnp.float32) + input_grad).astype(jnp.bfloat16)
        old_rows = lax.dynamic_index_in_dim(grad_stash, slot_index, 0, keepdims=False)
        grad_stash = lax.dynamic_update_index_in_dim(
            grad_stash, jnp.where(active, branch_gradient, old_rows), slot_index, 0
        )
        passed = passed_along(updated, "section", -1)
        return (passed, grad_stash, gain_grad)

    back_state = (
        jnp.zeros((block_rows, model_width), jnp.bfloat16),
        jnp.zeros((block_count, block_rows, model_width), jnp.bfloat16),
        jnp.zeros((model_width,), jnp.float32),
    )
    ignored, grad_stash, gain_grad = lax.fori_loop(0, tick_count, backward_tick, back_state)
    low_rows = low_stash.reshape(micro_count * token_count, rank_total)
    grad_rows = grad_stash.reshape(micro_count * token_count, model_width)
    grad_section = lax.dot_general(
        low_rows, grad_rows, (((0,), (0,)), ((), ())), preferred_element_type=jnp.float32
    )
    summed_up, summed_gain = lax.psum((grad_section, gain_grad), "dp")
    return (summed_up[None], summed_gain[None])


LANES = 128
PIECES = 8
EDGE = 3
PAIR = 2
VMEM_BUDGET = 24 * 1024 * 1024


def swapped(block, axis, bit):
    route = [(i, i ^ bit) for i in range(lax.axis_size(axis))]
    return lax.ppermute(block, axis, route)


def cross_product(left, right):
    return lax.dot_general(left, right, (((1,), (1,)), ((), ())), preferred_element_type=jnp.float32)


def pair_rows(rel, rank):
    return (rel // PAIR) * LANES + (rel % PAIR) * rank


def near_kernel(tokens_hbm, grads_hbm, own_hbm, other_hbm, stack, gram_ref, kept_ref, sems):
    rows = tokens_hbm.shape[0]
    rank = own_hbm.shape[0] // 2
    model_width = tokens_hbm.shape[1]
    piece = model_width // PIECES
    copies = []
    for p in range(PIECES):
        columns = pl.ds(p * piece, piece)
        moves = [(tokens_hbm, 0, 2 * LANES, rows), (grads_hbm, 0, 2 * LANES + rows, rows)]
        for j, source in enumerate((own_hbm, other_hbm)):
            for q in range(2):
                moves.append((source, q * rank, q * LANES + j * rank, rank))
        group = [
            pltpu.make_async_copy(
                source.at[pl.ds(from_row, count), columns],
                stack.at[pl.ds(to_row, count), columns],
                sems.at[p, i],
            )
            for i, (source, from_row, to_row, count) in enumerate(moves)
        ]
        for copy in group:
            copy.start()
        copies.append(group)
    flags = [
        pltpu.make_async_copy(
            source.at[pl.ds(0, 16), pl.ds(model_width, LANES)], kept_ref.at[j], sems.at[j, 6]
        )
        for j, source in enumerate((own_hbm, other_hbm))
    ]
    for copy in flags:
        copy.start()
    top = 2 * LANES + 2 * rows
    for base in (0, LANES, top, top + LANES):
        stack[base + PAIR * rank : base + LANES, :] = jnp.zeros(
            (LANES - PAIR * rank, model_width), jnp.bfloat16
        )
    joined = 2
    for p in range(0, PIECES, joined):
        for group in copies[p : p + joined]:
            for copy in group:
                copy.wait()
        columns = slice(p * piece, (p + joined) * piece)
        middle = (LANES + top) // 2
        for low, high in ((LANES, middle), (middle, top)):
            product = cross_product(stack[low:high, columns], stack[: 2 * LANES, columns])
            if p == 0:
                gram_ref[low - LANES : high - LANES, :] = product
            else:
                gram_ref[low - LANES : high - LANES, :] += product
        if p == 0:
            square = jnp.zeros((rows, LANES), jnp.float32)
        values = stack[2 * LANES : 2 * LANES + rows, columns].astype(jnp.float32)
        for j in range(joined * piece // LANES):
            part = values[:, j * LANES : (j + 1) * LANES]
            square += part * part
    gram_ref[top - LANES :, :LANES] = square
    gram_ref[top - LANES :, LANES:] = jnp.zeros((rows, LANES), jnp.float32)
    for copy in flags:
        copy.wait()


def rank_space_kernel(
    index_ref, valid_ref, near_gram_ref, near_kept_ref, *rest, regions, sections, rank, width,
    micro, tokens, parts
):
    sources = rest[: len(regions)]
    down, stack_in = rest[len(regions) : len(regions) + 2]
    payload_refs = rest[len(regions) + 2 : len(regions) + 2 + parts]
    stack, gram, proj, branch_stash, left_ref = rest[len(regions) + 2 + parts :]
    del stack_in
    rows = micro * tokens
    half = 2 * LANES
    top = half + 2 * rows
    model_width = stack.shape[1]
    piece = model_width // PIECES
    own = index_ref[0]
    side = index_ref[1]
    place = index_ref[2]
    near = pl.multiple_of(side * (PIECES - EDGE) * piece, LANES)
    away = pl.multiple_of((1 - side) * (PIECES - EDGE) * piece, LANES)
    offsets = {"near": near, "away": away, "middle": EDGE * piece}
    for source, (rel, matrices, where) in zip(sources, regions):
        lanes = (PIECES - 2 * EDGE if where == "middle" else EDGE) * piece
        for i, q in enumerate(matrices):
            base = top + (1 - q) * LANES + (rel % PAIR) * rank
            stack[base : base + rank, pl.ds(offsets[where], lanes)] = source[
                i * rank : (i + 1) * rank, :lanes
            ]
    steps = 4
    joined = model_width // steps
    middle = (top + LANES) // 2

    def far_products(p):
        columns = slice(p * joined, (p + 1) * joined)
        for low, high in ((0, middle), (middle, top + LANES)):
            product = cross_product(stack[low:high, columns], stack[top:, columns])
            if p == 0:
                proj[low:high, :] = product
            else:
                proj[low:high, :] += product

    for p in range(steps):
        pl.when(own >= 0)(functools.partial(far_products, p))
    down_near, down_far, up_near, up_far = [slice(i * LANES, (i + 1) * LANES) for i in range(4)]
    far_up, far_down = slice(0, LANES), slice(LANES, half)
    gram[:LANES, down_near] = near_gram_ref[:LANES, :LANES]
    gram[:LANES, up_near] = near_gram_ref[:LANES, LANES:]
    gram[:LANES, up_far] = proj[LANES:half, far_up]
    gram[:LANES, down_far] = proj[LANES:half, far_down]
    gram[LANES:, down_near] = proj[:LANES, far_up].T
    gram[LANES:, up_near] = proj[LANES:half, far_up].T
    gram[LANES:, up_far] = proj[top:, far_up]
    gram[LANES:, down_far] = proj[top:, far_down]
    norm_sq = jnp.sum(near_gram_ref[LANES + 2 * rows :, :LANES], axis=1, keepdims=True)
    token_near = near_gram_ref[LANES : LANES + rows, :]
    grad_near = near_gram_ref[LANES + rows : LANES + 2 * rows, :]
    token_far = proj[half : half + rows, :]
    grad_far = proj[half + rows : top, :]

    flag_rows = [near_kept_ref[j, 0:1, :].astype(jnp.float32) for j in range(PAIR)]
    for source, (rel, matrices, where) in zip(sources, regions):
        if where == "near" and matrices == (0,):
            flag_rows.append(source[0:16, EDGE * piece :].astype(jnp.float32)[0:1, :])
    ordered = []
    for s in range(sections):
        row = flag_rows[0]
        for j in range(1, sections):
            row = jnp.where((own ^ s) == j, flag_rows[j], row)
        ordered.append(row)
    ordered.append(valid_ref[...])
    ordered.append(jnp.zeros((LANES - len(ordered), rows), jnp.float32))
    masks = jnp.concatenate(ordered, axis=0).T
    lane_ids = lax.broadcasted_iota(jnp.int32, (rows, half), 1)
    firsts = [pair_rows(own ^ s, rank) for s in range(sections)]
    blocks = [(lane_ids >= first) & (lane_ids < first + rank) for first in firsts]
    kept = [masks[:, s : s + 1] for s in range(sections)]
    valid = masks[:, sections : sections + 1]
    gram_hi = gram[...].astype(jnp.bfloat16)
    gram_lo = (gram[...] - gram_hi.astype(jnp.float32)).astype(jnp.bfloat16)
    down_side = jnp.concatenate([token_near[:, :LANES], token_far[:, far_down]], axis=1)
    up_side = jnp.concatenate([token_near[:, LANES:], token_far[:, far_up]], axis=1)
    down_saved = jnp.zeros((rows, half), jnp.float32)
    kept_low = jnp.zeros((rows, half), jnp.float32)
    power = jnp.zeros((rows, 1), jnp.float32)
    count = jnp.zeros((rows, 1), jnp.float32)
    inverses = []
    for s in range(sections):
        inverse = lax.rsqrt(norm_sq / width + EPS)
        inverses.append(inverse)
        masked = jnp.where(blocks[s], down_side, 0.0)
        down_saved += masked
        low = (masked * inverse).astype(jnp.bfloat16)
        low_f32 = low.astype(jnp.float32)
        kept_low += kept[s] * low_f32
        branch_stash[s] = up_side
        moved = jnp.dot(low, gram_hi, preferred_element_type=jnp.float32) + jnp.dot(
            low, gram_lo, preferred_element_type=jnp.float32
        )
        energy = jnp.sum(low_f32 * moved[:, half:], axis=1, keepdims=True)
        cross = jnp.sum(low_f32 * up_side, axis=1, keepdims=True)
        power += kept[s] * energy
        count += kept[s]
        norm_sq = jnp.maximum(norm_sq + kept[s] * (2.0 * cross + energy), 0.0)
        down_side = down_side + kept[s] * moved[:, :half]
        up_side = up_side + kept[s] * moved[:, half:]

    def per_micro(column):
        wide = jnp.broadcast_to(column, (rows, LANES)).reshape(micro, tokens, LANES)
        total = jnp.broadcast_to(jnp.sum(wide, axis=1, keepdims=True), wide.shape)
        return total.reshape(rows, LANES)[:, :1]

    total_energy = jnp.maximum(per_micro(power), 0.0)
    total_count = per_micro(count)
    scaling = 1.0 / (total_count * jnp.sqrt(total_energy / (width * total_count) + EPS))
    alpha = valid * scaling

    carried = alpha * jnp.concatenate([grad_near[:, LANES:], grad_far[:, far_up]], axis=1)
    scaled_grad = jnp.zeros((rows, half), jnp.float32)
    later = jnp.zeros((rows, half), jnp.float32)
    weights = [None] * sections
    zero = jnp.zeros((rows, 1), jnp.float32)
    beta = zero
    for s in reversed(range(sections)):
        lowgrad = jnp.where(blocks[s], kept[s] * carried, 0.0).astype(jnp.bfloat16)
        lowgrad_f32 = lowgrad.astype(jnp.float32)
        mean = jnp.sum(lowgrad_f32 * down_saved, axis=1, keepdims=True) / width
        inverse = inverses[s]
        pull = inverse * inverse * inverse * mean
        weights[s] = pull
        scaled = inverse * lowgrad_f32
        scaled_grad += scaled
        if s > 0:
            back = lax.dot_general(
                lowgrad, gram_hi[:, :half], (((1,), (1,)), ((), ())), preferred_element_type=jnp.float32
            ) + lax.dot_general(
                lowgrad, gram_lo[:, :half], (((1,), (1,)), ((), ())), preferred_element_type=jnp.float32
            )
            carried = carried + inverse * back - pull * branch_stash[s]

    beta = zero
    gamma = jnp.zeros((rows, half), jnp.float32)
    after = jnp.zeros((rows, half), jnp.float32)
    before = jnp.zeros((rows, half), jnp.float32)
    for s in reversed(range(sections)):
        gamma = jnp.where(blocks[s], beta, gamma)
        beta = beta + jnp.where(s > own, weights[s], zero)
        after = jnp.where(blocks[s] & (s > own), scaled_grad, after)
        before = jnp.where(blocks[s] & (s < own), kept_low, before)
    after = after.astype(jnp.bfloat16)
    before = before.astype(jnp.bfloat16)
    pulled = (gamma * kept_low).astype(jnp.bfloat16)
    low_part = kept_low[:, :LANES]
    low_own = low_part.T[:rank].astype(jnp.bfloat16)
    grad_own = scaled_grad[:, :LANES].T[:rank].astype(jnp.bfloat16)
    from_grads = (alpha * low_part).T[:rank].astype(jnp.bfloat16)
    from_tokens = (-beta * low_part).T[:rank].astype(jnp.bfloat16)
    from_down = jnp.dot(low_own, after, preferred_element_type=jnp.float32).astype(jnp.bfloat16)
    from_up = -jnp.dot(low_own, pulled, preferred_element_type=jnp.float32).astype(jnp.bfloat16)
    gain_up = jnp.dot(grad_own, before, preferred_element_type=jnp.float32).astype(jnp.bfloat16)
    blank = jnp.zeros((rank, LANES), jnp.bfloat16)
    left = jnp.concatenate(
        [
            jnp.concatenate(
                [
                    from_down[:, :LANES], from_up[:, :LANES], from_tokens, from_grads,
                    from_up[:, LANES:], from_down[:, LANES:],
                ],
                axis=1,
            ),
            jnp.concatenate(
                [blank, gain_up[:, :LANES], grad_own, blank, gain_up[:, LANES:], blank], axis=1
            ),
        ],
        axis=0,
    )
    chunk = model_width // parts
    lane_blocks = chunk // LANES
    tail = payload_refs[0].shape[0] - lane_blocks * rank
    left_ref[...] = left

    def spread(k):
        columns = pl.ds(pl.multiple_of((place ^ k) * chunk, LANES), chunk)
        result = jnp.dot(left_ref[...], stack[:, columns], preferred_element_type=jnp.float32)
        gain = jnp.sum(
            result[rank:] * down[:, columns].astype(jnp.float32), axis=0, keepdims=True
        )
        for j in range(lane_blocks):
            payload_refs[k][j * rank : (j + 1) * rank, :] = result[
                :rank, j * LANES : (j + 1) * LANES
            ].astype(jnp.bfloat16)
        gain_rows = [gain[:, j * LANES : (j + 1) * LANES] for j in range(lane_blocks)]
        gain_rows.append(jnp.zeros((tail - lane_blocks, LANES), jnp.float32))
        payload_refs[k][lane_blocks * rank :, :] = jnp.concatenate(gain_rows, axis=0).astype(
            jnp.bfloat16
        )

    for k in reversed(range(parts)):
        pl.when(own >= 0)(functools.partial(spread, k))


def unpack_kernel(index_ref, *refs):
    parts_refs, (up_ref, gain_ref) = refs[:-2], refs[-2:]
    parts = len(parts_refs)
    rank = up_ref.shape[0]
    chunk = up_ref.shape[1] // parts
    lane_blocks = chunk // LANES
    for k in range(parts):
        start = (index_ref[2] ^ k) * chunk
        tail = parts_refs[k][lane_blocks * rank :, :].astype(jnp.float32)
        for j in range(lane_blocks):
            lanes = pl.ds(pl.multiple_of(start + j * LANES, LANES), LANES)
            up_ref[:, lanes] = parts_refs[k][j * rank : (j + 1) * rank, :].astype(jnp.float32)
            gain_ref[:, lanes] = tail[j : j + 1, :]


def summed(first, *others):
    total = first.astype(jnp.float32)
    for other in others:
        total = total + other.astype(jnp.float32)
    return total.astype(jnp.bfloat16)


def scattered_sum(blocks):
    parts = len(blocks)
    if parts == 1:
        return blocks[0]
    merged = {}
    for k in reversed(range(0, parts, 2)):
        merged[k] = summed(blocks[k], swapped(blocks[k + 1], "dp", 1))
    return summed(merged[0], *[swapped(merged[k], "dp", k) for k in reversed(range(2, parts, 2))])


def gathered_blocks(block):
    parts = lax.axis_size("dp")
    blocks = [block]
    if parts > 1:
        even = [block] + [swapped(block, "dp", k) for k in range(2, parts, 2)]
        blocks = [piece for one in even for piece in (one, swapped(one, "dp", 1))]
    return blocks


def rank_space_body(
    entry_tokens,
    section_norm_gain,
    adapter_down_weight,
    adapter_up_weight,
    output_gradient,
    lengths,
    keep,
):
    sections = lax.axis_size("section")
    parts = lax.axis_size("dp")
    section_index = lax.axis_index("section")
    micro, tokens, width = entry_tokens.shape[1:]
    rank = adapter_down_weight.shape[1]
    rows = micro * tokens
    down = adapter_down_weight[0]
    up = adapter_up_weight[0]
    place = lax.axis_index("dp")
    side = place & 1
    piece = width // PIECES
    edge = EDGE * piece
    near = side * (width - edge)
    up_edge = lax.dynamic_slice(up, (0, near), (rank, edge))
    up_edge, gain, keep = lax.optimization_barrier((up_edge, section_norm_gain, keep))
    valid = (jnp.arange(tokens, dtype=jnp.int32)[None, :] < lengths[0][:, None]).astype(jnp.float32)
    kept = (keep[0, 0].astype(jnp.float32) * valid).reshape(1, rows)
    flags = jnp.pad(kept.astype(jnp.bfloat16), ((0, rank - 1), (0, 0)))
    scaled_down = (
        gain.astype(jnp.float32) * down.astype(jnp.float32)
    ).astype(jnp.bfloat16)
    down_edge = jnp.concatenate(
        [lax.dynamic_slice(scaled_down, (0, near), (rank, edge)), flags], axis=1
    )
    weights = jnp.concatenate(
        [
            jnp.concatenate([scaled_down, flags], axis=1),
            jnp.pad(up, ((0, 0), (0, LANES))),
        ],
        axis=0,
    )
    middle = jnp.concatenate(
        [scaled_down[:, edge : width - edge], up[:, edge : width - edge]], axis=0
    )
    hbm = pl.BlockSpec(memory_space=pltpu.MemorySpace.HBM)
    vmem = pl.BlockSpec(memory_space=pltpu.MemorySpace.VMEM)
    smem = pl.BlockSpec(memory_space=pltpu.MemorySpace.SMEM)

    def on_chip(block):
        return pltpu.with_memory_space_constraint(block, pltpu.MemorySpace.VMEM)

    up_near = swapped(up_edge, "section", PAIR)
    down_near = swapped(down_edge, "section", PAIR)
    beside = swapped(weights, "section", 1)
    centre = swapped(middle, "section", PAIR)
    index = jnp.stack([section_index, side, place]).astype(jnp.int32)
    weights, index, valid = lax.optimization_barrier((weights, index, valid.reshape(1, rows)))
    stack_rows = 4 * LANES + 2 * rows
    stack, near_gram, near_kept = pl.pallas_call(
        near_kernel,
        out_shape=(
            pltpu.VMEM((stack_rows, width), jnp.bfloat16),
            pltpu.VMEM((LANES + 3 * rows, 2 * LANES), jnp.float32),
            pltpu.VMEM((PAIR, 16, LANES), jnp.bfloat16),
        ),
        in_specs=[hbm] * 4,
        out_specs=(vmem, vmem, vmem),
        scratch_shapes=[pltpu.SemaphoreType.DMA((PIECES, 7))],
        compiler_params=pltpu.CompilerParams(vmem_limit_bytes=VMEM_BUDGET),
        name="near_weights",
    )(
        pltpu.with_memory_space_constraint(
            entry_tokens.reshape(rows, width), pltpu.MemorySpace.HBM
        ),
        pltpu.with_memory_space_constraint(
            output_gradient.reshape(rows, width), pltpu.MemorySpace.HBM
        ),
        weights,
        beside,
    )
    up_away = swapped(up_near, "dp", 1)
    down_away = swapped(down_near, "dp", 1)
    regions = []
    sources = []
    for j in range(PAIR):
        regions += [
            (PAIR + j, (1,), "near"),
            (PAIR + j, (0,), "near"),
            (PAIR + j, (0, 1), "middle"),
            (PAIR + j, (1,), "away"),
            (PAIR + j, (0,), "away"),
        ]
    sources = [up_near, down_near, centre, up_away, down_away]
    sources += [swapped(block, "section", 1) for block in sources]
    lane_blocks = width // parts // LANES
    payload_rows = lane_blocks * rank + -(-lane_blocks // 16) * 16
    *payload, _ = pl.pallas_call(
        lambda *refs: rank_space_kernel(
            *refs,
            regions=regions,
            sections=sections,
            rank=rank,
            width=width,
            micro=micro,
            tokens=tokens,
            parts=parts,
        ),
        out_shape=[pltpu.VMEM((payload_rows, LANES), jnp.bfloat16)] * parts
        + [pltpu.VMEM((stack_rows, width), jnp.bfloat16)],
        in_specs=[smem] + [vmem] * (len(sources) + 5),
        out_specs=[vmem] * (parts + 1),
        input_output_aliases={len(sources) + 5: parts},
        scratch_shapes=[
            pltpu.VMEM((2 * LANES, 4 * LANES), jnp.float32),
            pltpu.VMEM((3 * LANES + 2 * rows, 2 * LANES), jnp.float32),
            pltpu.VMEM((sections, rows, 2 * LANES), jnp.float32),
            pltpu.VMEM((2 * rank, stack_rows), jnp.bfloat16),
        ],
        compiler_params=pltpu.CompilerParams(vmem_limit_bytes=VMEM_BUDGET),
        name="rank_space",
    )(
        index,
        valid,
        near_gram,
        near_kept,
        *[on_chip(block) for block in sources],
        on_chip(down),
        stack,
    )
    blocks = gathered_blocks(scattered_sum(payload))
    grad_up, grad_gain = pl.pallas_call(
        unpack_kernel,
        out_shape=(
            jax.ShapeDtypeStruct((rank, width), jnp.float32),
            jax.ShapeDtypeStruct((1, width), jnp.float32),
        ),
        in_specs=[smem] + [vmem] * parts,
        out_specs=(vmem, vmem),
        name="unpack",
    )(index, *[on_chip(block) for block in blocks])
    return (grad_up[None], grad_gain)


def fits_rank_space(args, sections, parts):
    micro, tokens, width = args[0].shape[1:]
    rank = args[2].shape[1]
    return (
        sections == 2 * PAIR
        and parts > 1
        and parts & (parts - 1) == 0
        and width % (parts * LANES) == 0
        and width % (PIECES * LANES) == 0
        and rank % 16 == 0
        and PAIR * rank <= LANES
        and micro * tokens == LANES
        and tokens % 8 == 0
        and 6 * LANES * width * 2 <= VMEM_BUDGET
    )


def body(*args):
    if fits_rank_space(args, lax.axis_size("section"), lax.axis_size("dp")):
        return rank_space_body(*args)
    return relay_body(*args)


def solution(mesh):
    in_specs = (
        P("dp", None, None, None),
        P("section", None),
        P("section", None, None),
        P("section", None, None),
        P("dp", None, None, None),
        P("dp", None),
        P("dp", "section", None, None),
    )
    out_specs = (P("section", None, None), P("section", None))
    return jax.shard_map(body, mesh=mesh, in_specs=in_specs, out_specs=out_specs, check_vma=False)
```
